8 devices in a mesh: data: 1 (over z), seq: 8 (over y, x, core).
Axes of the slice: x: 2, y: 2, z: 1, core: 2. Of those that a mesh axis runs over, the one named last changes fastest.
Arguments:
- x: bfloat16 [4096, 4096], P(('data', 'seq'))
- g: float32 [4096], replicated
- wqkv: bfloat16 [4096, 3, 16, 256], replicated
- wo: bfloat16 [16, 256, 4096], replicated
Outputs:
- output: bfloat16 [4096, 4096], P(('data', 'seq'))
All inputs are finite; a program needn't handle non-finite values.
Results may differ from the reference program's by a relative error of at most 0.00306945.
Values are sent between devices in bfloat16 or wider.
A program may use at most 1 GiB of HBM per device.

```python
import jax
import jax.numpy as jnp
from jax import lax

S = 4096
D = 4096
HEADS = 16
HEAD = 256


def setup_inputs(seed: int = 0, part: int = 0) -> dict:
    k_shared, k_part = jax.random.split(jax.random.PRNGKey(seed))
    kx, kf, ku = jax.random.split(jax.random.fold_in(k_part, part), 3)
    kg, kq, ko = jax.random.split(k_shared, 3)
    r = jnp.arange(S, dtype=jnp.float32)[:, None] / S
    freq = jnp.array([0.5, 1.0, 1.5, 2.5], jnp.float32)
    phase = jax.random.uniform(kf, (4,), jnp.float32, 0.0, 2.0 * jnp.pi)
    waves = jnp.sin(2.0 * jnp.pi * r * freq + phase)
    u = jax.random.normal(ku, (4, D), jnp.float32)
    x = 0.25 * jax.random.normal(kx, (S, D), jnp.float32) + 0.35 * (waves @ u)
    g = 1.0 + 0.2 * jax.random.normal(kg, (D,), jnp.float32)
    wqkv = jax.random.normal(kq, (D, 3, HEADS, HEAD), jnp.float32) * D ** -0.5
    wo = jax.random.normal(ko, (HEADS, HEAD, D), jnp.float32) * (HEADS * HEAD) ** -0.5
    return {"x": x.astype(jnp.bfloat16), "g": g, "wqkv": wqkv.astype(jnp.bfloat16), "wo": wo.astype(jnp.bfloat16)}


def _rope(x, pos):
    half = HEAD // 2
    inv = 10000.0 ** (-jnp.arange(half, dtype=jnp.float32) * 2.0 / HEAD)
    ang = pos[:, None] * inv[None, :]
    cos = jnp.cos(ang)[:, None, :]
    sin = jnp.sin(ang)[:, None, :]
    x1, x2 = x[..., :half], x[..., half:]
    return jnp.concatenate([x1 * cos - x2 * sin, x2 * cos + x1 * sin], axis=-1)


def reference(x, g, wqkv, wo):
    xf = x.astype(jnp.float32)
    xn = (xf * lax.rsqrt(jnp.mean(xf * xf, axis=-1, keepdims=True) + 1e-5) * g).astype(jnp.bfloat16)
    qkv = jnp.dot(xn, wqkv.reshape(D, 3 * HEADS * HEAD), preferred_element_type=jnp.float32).reshape(S, 3, HEADS, HEAD)
    pos = jnp.arange(S, dtype=jnp.float32)
    q = _rope(qkv[:, 0], pos).astype(jnp.bfloat16)
    k = _rope(qkv[:, 1], pos).astype(jnp.bfloat16)
    v = qkv[:, 2].astype(jnp.bfloat16)
    qb = min(S, 512)
    nq = S // qb
    scale = HEAD ** -0.5

    def one_head(args):
        qh, kh, vh = args

        def one_block(a):
            qblk, i = a
            sc = jnp.dot(qblk, kh.T, preferred_element_type=jnp.float32) * scale
            mask = (i * qb + jnp.arange(qb))[:, None] >= jnp.arange(S)[None, :]
            sc = jnp.where(mask, sc, -jnp.inf)
            pr = jax.nn.softmax(sc, axis=-1).astype(jnp.bfloat16)
            return jnp.dot(pr, vh, preferred_element_type=jnp.float32).astype(jnp.bfloat16)

        o = lax.map(one_block, (qh.reshape(nq, qb, HEAD), jnp.arange(nq)))
        return o.reshape(S, HEAD)

    o = lax.map(one_head, (q.transpose(1, 0, 2), k.transpose(1, 0, 2), v.transpose(1, 0, 2)))
    o = o.transpose(1, 0, 2).reshape(S, HEADS * HEAD)
    y = xf + jnp.dot(o, wo.reshape(HEADS * HEAD, D), preferred_element_type=jnp.float32)
    return y.astype(jnp.bfloat16)
```

```python
import functools

import jax
import jax.numpy as jnp
from jax import lax
from jax.experimental import pallas as pl
from jax.experimental.pallas import tpu as pltpu
from jax.sharding import PartitionSpec as P

BF = jnp.bfloat16
F32 = jnp.float32
VMEM_LIMIT = 62 << 20


def _norm(x_ref, g_ref, xn):
    rb = 64

    def body(i, c):
        r = pl.ds(pl.multiple_of(i * rb, rb), rb)
        xf = x_ref[r, :].astype(F32)
        ms = jnp.mean(xf * xf, axis=-1, keepdims=True)
        xn[r, :] = (xf * lax.rsqrt(ms + 1e-5) * g_ref[...]).astype(BF)
        return c

    lax.fori_loop(0, x_ref.shape[0] // rb, body, 0)


def _rope_store(a, cos, sin, is_v, o_ref, h):
    half = a.shape[-1] // 2
    x1, x2 = a[:, :half], a[:, half:]
    c = jnp.where(is_v, 1.0, cos)
    s = jnp.where(is_v, 0.0, sin)
    o_ref[0, h, :, :half] = (x1 * c - x2 * s).astype(BF)
    o_ref[0, h, :, half:] = (x2 * c + x1 * s).astype(BF)


def _qkv_first(idx, x_ref, g_ref, w_ref, cos_ref, sin_ref, s_ref, c_ref, wr_ref, xn, acc, wt):
    c, d = pl.program_id(0), pl.program_id(1)
    nd = pl.num_programs(1)
    bd = w_ref.shape[0]

    @pl.when((c == 0) & (d == 0))
    def _():
        _norm(x_ref, g_ref, xn)

    @pl.when(d == 0)
    def _():
        acc[...] = jnp.zeros_like(acc)

    wt[...] = jnp.swapaxes(w_ref[:, 0], 0, 1)
    xb = xn[:, pl.ds(pl.multiple_of(d * bd, bd), bd)]
    for j in range(4):
        wr_ref[0, j] = wt[idx[1 + j]]
        acc[:, j * 256:(j + 1) * 256] += jnp.dot(xb, wr_ref[0, j], preferred_element_type=F32)

    @pl.when(d == nd - 1)
    def _():
        cos, sin = cos_ref[...], sin_ref[...]
        for j in range(4):
            o = s_ref if j < 2 else c_ref
            _rope_store(acc[:, j * 256:(j + 1) * 256], cos, sin, c == 2, o, j % 2)


def _qkv_next(x_ref, g_ref, w_ref, cos_ref, sin_ref, s_ref, c_ref, xn):
    c, j = pl.program_id(0), pl.program_id(1)

    @pl.when((c == 0) & (j == 0))
    def _():
        _norm(x_ref, g_ref, xn)

    def emit(o_ref):
        cos, sin = cos_ref[...], sin_ref[...]
        for h in range(2):
            a = jnp.dot(xn[...], w_ref[0, h], preferred_element_type=F32)
            _rope_store(a, cos, sin, c == 2, o_ref, h)

    @pl.when(j == 0)
    def _():
        emit(s_ref)

    @pl.when(j == 1)
    def _():
        emit(c_ref)


def _attend(nq, ids, *refs):
    src, outs = refs[:8], refs[8:8 + nq]
    qkv, m_s, l_s, acc, sem = refs[8 + nq:]
    t, dh = src[0].shape[2:]
    cps = []
    for n in range(8):
        rows = pl.ds(pl.multiple_of(ids[n] * t, t), t)
        cp = pltpu.make_async_copy(src[n], qkv.at[:, :, rows, :], sem.at[n])
        cp.start()
        cps.append(cp)
    for cp in cps:
        cp.wait()
    k2 = (dh ** -0.5) * 1.4426950408889634

    for n in range(nq):
        r = ids[8 + n]
        qrows = pl.ds(pl.multiple_of(r * t, t), t)
        m_s[...] = jnp.full_like(m_s, -jnp.inf)
        l_s[...] = jnp.zeros_like(l_s)
        acc[...] = jnp.zeros_like(acc)

        def block(j, diag):
            krows = pl.ds(pl.multiple_of(j * t, t), t)
            for h in range(2):
                s = lax.dot_general(qkv[0, h, qrows, :], qkv[1, h, krows, :], (((1,), (1,)), ((), ())),
                                    preferred_element_type=F32)
                if diag:
                    row = lax.broadcasted_iota(jnp.int32, (t, t), 0)
                    col = lax.broadcasted_iota(jnp.int32, (t, t), 1)
                    s = jnp.where(row >= col, s, -jnp.inf)
                m_old = m_s[h]
                m_new = jnp.maximum(m_old, jnp.max(s, axis=-1, keepdims=True))
                alpha = jnp.exp2((m_old - m_new) * k2)
                p = jnp.exp2((s - m_new[:, :1]) * k2)
                ls = p[:, :128]
                for q in range(1, t // 128):
                    ls = ls + p[:, q * 128:(q + 1) * 128]
                l_s[h] = l_s[h] * alpha + ls
                pv = jnp.dot(p.astype(BF), qkv[2, h, krows, :], preferred_element_type=F32)
                acc[h] = acc[h] * alpha[:, :1] + pv
                m_s[h] = m_new

        def body(j, c):
            block(j, False)
            return c

        lax.fori_loop(0, r, body, 0)
        block(r, True)
        for h in range(2):
            l = jnp.sum(l_s[h], axis=-1, keepdims=True)
            outs[n][:, h * dh:(h + 1) * dh] = (acc[h] / l).astype(BF)


def _out_first(idx, *refs):
    n = (len(refs) - 1) // 2
    o, w, out = refs[:n], refs[n:2 * n], refs[-1]
    a = jnp.dot(o[0][...], w[0][...], preferred_element_type=F32)
    for i in range(1, n):
        a = a + jnp.dot(o[i][...], w[i][...], preferred_element_type=F32)
    out[...] = a


def _out_last(idx, *refs):
    n = (len(refs) - 3) // 2
    o, w, part, x, out = refs[:n], refs[n:2 * n], refs[2 * n], refs[2 * n + 1], refs[-1]
    a = part[...]
    for i in range(n):
        a = a + jnp.dot(o[i][...], w[i][...], preferred_element_type=F32)
    out[...] = (x[...].astype(F32) + a).astype(BF)


def _params(**kw):
    return pltpu.CompilerParams(vmem_limit_bytes=VMEM_LIMIT, **kw)


def _cost(flops, nbytes):
    return pl.CostEstimate(flops=int(flops), bytes_accessed=int(nbytes), transcendentals=0)


def solution(mesh):
    rows = P(("data", "seq"), None)

    def local(x, g, wqkv, wo):
        t, d = x.shape
        _, _, hh, dh = wqkv.shape
        me = lax.axis_index("seq").astype(jnp.int32)
        k = me % 2
        kf, yf = 2 << k, 4 >> k

        def perm(f):
            pairs = [(i, f(i)) for i in range(8)]
            return lambda a: lax.ppermute(a, "seq", pairs)

        to_a = perm(lambda i: i ^ (2 << (i & 1)))
        to_same = perm(lambda i: i ^ (4 >> (i & 1)))
        to_cross = perm(lambda i: i ^ (4 >> (i & 1)) ^ 1)
        to_p = perm(lambda i: i ^ 1)

        inv = 10000.0 ** (-jnp.arange(dh // 2, dtype=F32) * 2.0 / dh)

        def tables(b):
            ang = (b * t + jnp.arange(t)).astype(F32)[:, None] * inv[None, :]
            return jnp.cos(ang), jnp.sin(ang)

        cos_o, sin_o = tables(me)
        a_id = me ^ kf
        cos_a, sin_a = tables(a_id)
        g2 = g[None, :]

        xa = to_a(x)

        half = jax.ShapeDtypeStruct((3, 2, t, dh), BF)
        bd = 1024
        row_spec = pl.BlockSpec((t, d), lambda c, i, *_: (0, 0), pipeline_mode=pl.Buffered(1))
        g_spec = pl.BlockSpec((1, d), lambda c, i, *_: (0, 0))
        tab_spec = pl.BlockSpec((t, dh // 2), lambda c, i, *_: (0, 0))
        half_spec = pl.BlockSpec((1, 2, t, dh), lambda c, i, *_: (c, 0, 0, 0))
        flops = 2 * t * d * 12 * dh

        def first(chip):
            tile, off = chip // 2, (chip % 2) * 4
            base = jnp.stack([tile, off + 2 * k, off + 2 * k + 1, off + 2 - 2 * k, off + 3 - 2 * k])
            return pl.pallas_call(
                _qkv_first,
                grid_spec=pltpu.PrefetchScalarGridSpec(
                    num_scalar_prefetch=1, grid=(3, d // bd),
                    in_specs=[row_spec, g_spec,
                              pl.BlockSpec((bd, 1, 8, dh), lambda c, i, s: (i, c, s[0], 0)),
                              tab_spec, tab_spec],
                    out_specs=[half_spec, half_spec,
                               pl.BlockSpec((1, 4, bd, dh), lambda c, i, s: (c, 0, i, 0))],
                    scratch_shapes=[pltpu.VMEM((t, d), BF), pltpu.VMEM((t, 4 * dh), F32),
                                    pltpu.VMEM((8, bd, dh), BF)]),
                out_shape=[half, half, jax.ShapeDtypeStruct((3, 4, d, dh), BF)],
                compiler_params=_params(), cost_estimate=_cost(flops * 2, 80e6),
            )(base.astype(jnp.int32), x, g2, wqkv, cos_o, sin_o)

        def following(w):
            return pl.pallas_call(
                _qkv_next,
                grid=(3, 2),
                in_specs=[row_spec, g_spec,
                          pl.BlockSpec((1, 2, d, dh), lambda c, i: (c, i, 0, 0)),
                          tab_spec, tab_spec],
                out_specs=[half_spec, half_spec],
                out_shape=[half, half],
                scratch_shapes=[pltpu.VMEM((t, d), BF)],
                compiler_params=_params(), cost_estimate=_cost(flops * 1.4, 35e6),
            )(xa, g2, w, cos_a, sin_a)

        chip = me // 2
        b_same, b_cross, w_b = first((me ^ yf) // 2)
        rs_own, rc_own = to_same(b_same), to_cross(b_cross)
        l_own, p_own, w_o = first(chip)
        rp_own = to_p(p_own)
        a_same, a_cross = following(w_b)
        rs_a, rc_a = to_same(a_same), to_cross(a_cross)
        l_a, p_a = following(w_o)
        rp_a = to_p(p_a)

        po = me ^ 1
        so = me ^ yf
        xo = me ^ 1 ^ (2 << k)
        src = [l_own, l_a, rp_own, rp_a, rs_own, rs_a, rc_own, rc_a]
        ids = [me, a_id, po, po ^ (4 >> k), so, me ^ 6, xo, me ^ 7]

        def attend(ms):
            nq = len(ms)
            sc = jnp.stack(ids + [me ^ m for m in ms]).astype(jnp.int32)
            anyspec = pl.BlockSpec(memory_space=pl.ANY)
            return pl.pallas_call(
                functools.partial(_attend, nq),
                grid_spec=pltpu.PrefetchScalarGridSpec(
                    num_scalar_prefetch=1, grid=(1,),
                    in_specs=[anyspec] * 8,
                    out_specs=[pl.BlockSpec((t, 2 * dh), lambda i, s: (0, 0))] * nq,
                    scratch_shapes=[pltpu.VMEM((3, 2, 8 * t, dh), BF),
                                    pltpu.VMEM((2, t, 128), F32), pltpu.VMEM((2, t, 128), F32),
                                    pltpu.VMEM((2, t, dh), F32), pltpu.SemaphoreType.DMA((8,))]),
                out_shape=[jax.ShapeDtypeStruct((t, 2 * dh), BF)] * nq,
                compiler_params=_params(), cost_estimate=_cost(nq * 6e9, 13e6),
            )(sc, *src)

        order = ((6, 7), (2, 3, 4, 5), (1, 0))
        got = {}
        for ms in order:
            for m, o in zip(ms, attend(ms)):
                got[m] = perm(lambda i, m=m: i ^ m)(o) if m else o

        wo2 = wo.reshape(hh * dh, d)
        tn = 1024
        o_spec = pl.BlockSpec((t, 2 * dh), lambda i, s: (0, 0))

        def w_spec(n):
            return pl.BlockSpec((2 * dh, tn), lambda i, s: (s[n], i))

        def project(ms, part=None):
            n = len(ms)
            sc = jnp.stack([me ^ m for m in ms]).astype(jnp.int32)
            col = pl.BlockSpec((t, tn), lambda i, s: (0, i))
            extra = [] if part is None else [part, x]
            return pl.pallas_call(
                _out_first if part is None else _out_last,
                grid_spec=pltpu.PrefetchScalarGridSpec(
                    num_scalar_prefetch=1, grid=(d // tn,),
                    in_specs=[o_spec] * n + [w_spec(i) for i in range(n)] + [col] * len(extra),
                    out_specs=col),
                out_shape=jax.ShapeDtypeStruct((t, d), F32 if part is None else BF),
                compiler_params=_params(), cost_estimate=_cost(n * 2 * t * 2 * dh * d * 1.3, n * 4.2e6 + 8e6),
            )(sc, *[got[m] for m in ms], *[wo2] * n, *extra)

        part = project((6, 7, 1, 0))
        return project((2, 3, 4, 5), part)

    return jax.shard_map(local, mesh=mesh,
                         in_specs=(rows, P(None), P(None, None, None, None), P(None, None, None)),
                         out_specs=rows, check_vma=False)
```

```python
import functools

import jax
import jax.numpy as jnp
from jax import lax
from jax.experimental import pallas as pl
from jax.experimental.pallas import tpu as pltpu
from jax.sharding import PartitionSpec as P


BF = jnp.bfloat16
F32 = jnp.float32
VMEM_LIMIT = 62 << 20
COST = 0.05
GROUPS = ((6,), (2, 4), (0,))
ME, B_TILE, B_HEADS, OWN_TILE, OWN_HEADS, SRC, DEV = 0, 1, 2, 6, 7, 11, 19


def _norm(x_ref, g_ref, xn, base):
    rb = 64

    def body(i, c):
        r = pl.ds(pl.multiple_of(i * rb, rb), rb)
        xf = x_ref[r, :].astype(F32)
        ms = jnp.mean(xf * xf, axis=-1, keepdims=True)
        xn[pl.ds(pl.multiple_of(base + i * rb, rb), rb), :] = (xf * lax.rsqrt(ms + 1e-5) * g_ref[...]).astype(BF)
        return c

    lax.fori_loop(0, x_ref.shape[0] // rb, body, 0)


def _rope_store(a, cos, sin, is_v, o_ref):
    half = a.shape[-1] // 2
    x1, x2 = a[:, :half], a[:, half:]
    c = jnp.where(is_v, 1.0, cos)
    s = jnp.where(is_v, 0.0, sin)
    o_ref[:, :half] = (x1 * c - x2 * s).astype(BF)
    o_ref[:, half:] = (x2 * c + x1 * s).astype(BF)


def _relayout_dot(idx, w_ref, wt, xb, acc, wr_ref=None):
    wt[...] = jnp.swapaxes(w_ref[:, 0], 0, 1)
    ws = [wt[i] for i in idx]
    if wr_ref is not None:
        for j in range(4):
            wr_ref[0, j] = ws[j]
    acc[...] += jnp.dot(xb, jnp.concatenate(ws, axis=1), preferred_element_type=F32)


def _qkv_first(ids, x_ref, g_ref, w_ref, cos_ref, sin_ref, s_ref, c_ref, wr_ref, xn, acc, wt):
    c, d = pl.program_id(0), pl.program_id(1)
    bd = w_ref.shape[0]

    @pl.when((c == 0) & (d == 0))
    def _():
        _norm(x_ref, g_ref, xn, 0)

    @pl.when(d == 0)
    def _():
        acc[...] = jnp.zeros_like(acc)

    xb = xn[:, pl.ds(pl.multiple_of(d * bd, bd), bd)]
    _relayout_dot([ids[B_HEADS + j] for j in range(4)], w_ref, wt, xb, acc, wr_ref)

    @pl.when(d == pl.num_programs(1) - 1)
    def _():
        cos, sin = cos_ref[...], sin_ref[...]
        for j in range(4):
            o = s_ref if j < 2 else c_ref
            _rope_store(acc[:, j * 256:(j + 1) * 256], cos, sin, c == 2, o.at[0, j % 2])


def _qkv_next(x_ref, g_ref, w_ref, cos_ref, sin_ref, s_ref, c_ref, xn):
    c, j = pl.program_id(0), pl.program_id(1)

    @pl.when((c == 0) & (j == 0))
    def _():
        _norm(x_ref, g_ref, xn, 0)

    def emit(o_ref):
        cos, sin = cos_ref[...], sin_ref[...]
        w = jnp.concatenate([w_ref[0, 0], w_ref[0, 1]], axis=1)
        a = jnp.dot(xn[...], w, preferred_element_type=F32)
        for h in range(2):
            _rope_store(a[:, h * 256:(h + 1) * 256], cos, sin, c == 2, o_ref.at[0, h])

    @pl.when(j == 0)
    def _():
        emit(s_ref)

    @pl.when(j == 1)
    def _():
        emit(c_ref)


def _qkv_own(ids, x_ref, xa_ref, g_ref, w_ref, cos_ref, sin_ref, l_ref, p_ref, xn, acc, wt):
    c, d = pl.program_id(0), pl.program_id(1)
    bd = w_ref.shape[0]
    t = x_ref.shape[0]

    @pl.when((c == 0) & (d == 0))
    def _():
        _norm(x_ref, g_ref, xn, 0)
        _norm(xa_ref, g_ref, xn, t)

    @pl.when(d == 0)
    def _():
        acc[...] = jnp.zeros_like(acc)

    xb = xn[:, pl.ds(pl.multiple_of(d * bd, bd), bd)]
    _relayout_dot([ids[OWN_HEADS + j] for j in range(4)], w_ref, wt, xb, acc)

    @pl.when(d == pl.num_programs(1) - 1)
    def _():
        for b in range(2):
            r = slice(b * t, (b + 1) * t)
            cos, sin = cos_ref[r], sin_ref[r]
            for j in range(4):
                o = l_ref if j < 2 else p_ref
                _rope_store(acc[r, j * 256:(j + 1) * 256], cos, sin, c == 2, o.at[b, 0, j % 2])


def _attend(masks, ids, l_ref, rp_ref, rs0, rs1, rc0, rc1, *refs):
    nq = len(masks)
    outs = refs[:2 * nq]
    qkv, m_s, l_s, acc, sem = refs[2 * nq:]
    src = [l_ref.at[0], l_ref.at[1], rp_ref.at[0], rp_ref.at[1], rs0, rs1, rc0, rc1]
    t, dh = rs0.shape[2:]
    me = ids[ME]
    chips = [(me ^ m) // 2 for m in masks]
    last = functools.reduce(jnp.maximum, chips)

    def kv_copy(n, b):
        rows = pl.ds(pl.multiple_of(b * t, t), t)
        return pltpu.make_async_copy(src[n].at[pl.ds(1, 2)], qkv.at[pl.ds(1, 2), :, rows, :], sem.at[0, b])

    def q_copy(n, b):
        rows = pl.ds(pl.multiple_of(b * t, t), t)
        return pltpu.make_async_copy(src[n].at[0], qkv.at[0, :, rows, :], sem.at[1, b])

    for n in range(8):
        b = ids[SRC + n]
        want = functools.reduce(jnp.logical_or, [b // 2 == cc for cc in chips])

        @pl.when(want)
        def _():
            q_copy(n, b).start()

        @pl.when(b // 2 <= last)
        def _():
            kv_copy(n, b).start()

    k2 = (dh ** -0.5) * 1.4426950408889634

    for i in range(nq):
        cc = chips[i]
        q0 = pl.multiple_of(cc * 2 * t, 2 * t)
        for b in range(2):
            q_copy(0, 2 * cc + b).wait()
        m_s[...] = jnp.full_like(m_s, -jnp.inf)
        l_s[...] = jnp.zeros_like(l_s)
        acc[...] = jnp.zeros_like(acc)

        def kv_wait(j):
            if i == 0:
                for b in range(2):
                    kv_copy(0, 2 * j + b).wait()

        def tile(base, r0, nr, w, masked):
            rs = slice(r0, r0 + nr)
            ss = []
            for h in range(2):
                s = lax.dot_general(qkv[0, h, pl.ds(q0 + r0, nr), :], qkv[1, h, pl.ds(base, w), :],
                                    (((1,), (1,)), ((), ())), preferred_element_type=F32)
                if masked:
                    row = lax.broadcasted_iota(jnp.int32, (nr, w), 0)
                    col = lax.broadcasted_iota(jnp.int32, (nr, w), 1)
                    s = jnp.where(row >= col, s, -jnp.inf)
                ss.append(s)
            for h in range(2):
                ch = [ss[h][:, q * 128:(q + 1) * 128] for q in range(w // 128)]
                m_old = m_s[h, rs]
                m_new = jnp.maximum(m_old, jnp.max(functools.reduce(jnp.maximum, ch), axis=-1, keepdims=True))
                alpha = jnp.exp2((m_old - m_new) * k2)
                m_s[h, rs] = m_new
                mk = m_new * k2
                ps = [jnp.exp2(v * k2 - mk) for v in ch]
                l_s[h, rs] = l_s[h, rs] * alpha + functools.reduce(jnp.add, ps)
                p = jnp.concatenate([v.astype(BF) for v in ps], axis=1)
                pv = jnp.dot(p, qkv[2, h, pl.ds(base, w), :], preferred_element_type=F32)
                for q in range(dh // 128):
                    sl = slice(q * 128, (q + 1) * 128)
                    acc[h, rs, sl] = acc[h, rs, sl] * alpha + pv[:, sl]

        def body(j, carry):
            kv_wait(j)
            tile(pl.multiple_of(j * 2 * t, 2 * t), 0, 2 * t, 2 * t, False)
            return carry

        lax.fori_loop(0, cc, body, 0)
        kv_wait(cc)
        tile(q0, 0, t, t, True)
        tile(q0, t, t, t, False)
        tile(pl.multiple_of(q0 + t, t), t, t, t, True)
        if i == 0 and nq > 1:
            def drain(j, carry):
                kv_wait(j)
                return carry

            lax.fori_loop(cc + 1, last + 1, drain, 0)
        k = me % 2
        for o in range(2):
            rs = pl.ds(pl.multiple_of((k if o == 0 else 1 - k) * t, t), t)
            for h in range(2):
                l = jnp.sum(l_s[h, rs, :], axis=-1, keepdims=True)
                outs[2 * i + o][:, h * dh:(h + 1) * dh] = (acc[h, rs, :] / l).astype(BF)


def _out_first(ids, *refs):
    n = (len(refs) - 1) // 2
    o = jnp.concatenate([r[...] for r in refs[:n]], axis=1)
    w = jnp.concatenate([r[...] for r in refs[n:2 * n]], axis=0)
    refs[-1][...] = jnp.dot(o, w, preferred_element_type=F32)


def _out_last(ids, *refs):
    n = (len(refs) - 3) // 2
    o = jnp.concatenate([r[...] for r in refs[:n]], axis=1)
    w = jnp.concatenate([r[...] for r in refs[n:2 * n]], axis=0)
    part, x, out = refs[2 * n], refs[2 * n + 1], refs[-1]
    a = part[...] + jnp.dot(o, w, preferred_element_type=F32)
    out[...] = (x[...].astype(F32) + a).astype(BF)


def _params(**kw):
    return pltpu.CompilerParams(vmem_limit_bytes=VMEM_LIMIT, **kw)


def _cost(flops, nbytes):
    return pl.CostEstimate(flops=int(flops * COST), bytes_accessed=int(nbytes * COST), transcendentals=0)


def solution(mesh):
    rows = P(("data", "seq"), None)

    def local(x, g, wqkv, wo):
        t, d = x.shape
        _, _, hh, dh = wqkv.shape
        me = lax.axis_index("seq").astype(jnp.int32)
        k = me % 2
        kf, yf = 2 << k, 4 >> k

        def send(a, f):
            return lax.ppermute(a, "seq", [(i, f(i)) for i in range(8)])

        def to_a(i):
            return i ^ (2 << (i & 1))

        def to_same(i):
            return i ^ (4 >> (i & 1))

        def to_cross(i):
            return to_same(i) ^ 1

        inv = 10000.0 ** (-jnp.arange(dh // 2, dtype=F32) * 2.0 / dh)

        def tables(b):
            pos = (b[:, None] * t + jnp.arange(t)[None, :]).reshape(-1).astype(F32)
            ang = pos[:, None] * inv[None, :]
            return jnp.cos(ang), jnp.sin(ang)

        chip, a_id, so, po = me // 2, me ^ kf, me ^ yf, me ^ 1
        xo = po ^ kf

        def heads(ch):
            off = (ch % 2) * 4
            return [ch // 2, off + 2 * k, off + 2 * k + 1, off + 2 - 2 * k, off + 3 - 2 * k]

        ids = jnp.stack([me] + heads(so // 2) + heads(chip)
                        + [me, a_id, po, po ^ yf, so, me ^ 6, xo, me ^ 7]
                        + [me ^ m for m in range(8)]).astype(jnp.int32)
        cos, sin = tables(jnp.stack([me, a_id]))
        g2 = g[None, :]

        xa = send(x, to_a)

        half = jax.ShapeDtypeStruct((3, 2, t, dh), BF)
        both = jax.ShapeDtypeStruct((2, 3, 2, t, dh), BF)
        bd = 1024
        row_spec = pl.BlockSpec((t, d), lambda c, i, *_: (0, 0), pipeline_mode=pl.Buffered(1))
        g_spec = pl.BlockSpec((1, d), lambda c, i, *_: (0, 0))
        half_spec = pl.BlockSpec((1, 2, t, dh), lambda c, i, *_: (c, 0, 0, 0))
        both_spec = pl.BlockSpec((2, 1, 2, t, dh), lambda c, i, *_: (0, c, 0, 0, 0))
        flops = 2 * t * d * 12 * dh

        def tab_spec(b):
            return pl.BlockSpec((t, dh // 2), lambda c, i, *_: (b, 0))

        both_tab = pl.BlockSpec((2 * t, dh // 2), lambda c, i, *_: (0, 0))

        def tile_spec(at):
            return pl.BlockSpec((bd, 1, 8, dh), lambda c, i, s: (i, c, s[at], 0))

        b_same, b_cross, w_b = pl.pallas_call(
            _qkv_first,
            grid_spec=pltpu.PrefetchScalarGridSpec(
                num_scalar_prefetch=1, grid=(3, d // bd),
                in_specs=[row_spec, g_spec, tile_spec(B_TILE), tab_spec(0), tab_spec(0)],
                out_specs=[half_spec, half_spec, pl.BlockSpec((1, 4, bd, dh), lambda c, i, s: (c, 0, i, 0))],
                scratch_shapes=[pltpu.VMEM((t, d), BF), pltpu.VMEM((t, 4 * dh), F32),
                                pltpu.VMEM((8, bd, dh), BF)]),
            out_shape=[half, half, jax.ShapeDtypeStruct((3, 4, d, dh), BF)],
            compiler_params=_params(), cost_estimate=_cost(flops * 2.5, 80e6), name="qkv_first",
        )(ids, x, g2, wqkv, cos, sin)
        rs_own, rc_own = send(b_same, to_same), send(b_cross, to_cross)
        a_same, a_cross = pl.pallas_call(
            _qkv_next,
            grid=(3, 2),
            in_specs=[row_spec, g_spec, pl.BlockSpec((1, 2, d, dh), lambda c, i: (c, i, 0, 0)),
                      tab_spec(1), tab_spec(1)],
            out_specs=[half_spec, half_spec],
            out_shape=[half, half],
            scratch_shapes=[pltpu.VMEM((t, d), BF)],
            compiler_params=_params(), cost_estimate=_cost(flops * 1.4, 35e6), name="qkv_next",
        )(xa, g2, w_b, cos, sin)
        rs_a, rc_a = send(a_same, to_same), send(a_cross, to_cross)
        loc, par = pl.pallas_call(
            _qkv_own,
            grid_spec=pltpu.PrefetchScalarGridSpec(
                num_scalar_prefetch=1, grid=(3, d // bd),
                in_specs=[row_spec, row_spec, g_spec, tile_spec(OWN_TILE), both_tab, both_tab],
                out_specs=[both_spec, both_spec],
                scratch_shapes=[pltpu.VMEM((2 * t, d), BF), pltpu.VMEM((2 * t, 4 * dh), F32),
                                pltpu.VMEM((8, bd, dh), BF)]),
            out_shape=[both, both],
            compiler_params=_params(), cost_estimate=_cost(flops * 2.8, 60e6), name="qkv_own",
        )(ids, x, xa, g2, wqkv, cos, sin)
        rpar = send(par, lambda i: i ^ 1)
        src = [loc, rpar, rs_own, rs_a, rc_own, rc_a]

        def attend(ms):
            nq = len(ms)
            anyspec = pl.BlockSpec(memory_space=pl.ANY)
            return pl.pallas_call(
                functools.partial(_attend, ms),
                grid_spec=pltpu.PrefetchScalarGridSpec(
                    num_scalar_prefetch=1, grid=(1,),
                    in_specs=[anyspec] * 6,
                    out_specs=[pl.BlockSpec((t, 2 * dh), lambda i, s: (0, 0))] * (2 * nq),
                    scratch_shapes=[pltpu.VMEM((3, 2, 8 * t, dh), BF),
                                    pltpu.VMEM((2, 2 * t, 128), F32), pltpu.VMEM((2, 2 * t, 128), F32),
                                    pltpu.VMEM((2, 2 * t, dh), F32), pltpu.SemaphoreType.DMA((2, 8))]),
                out_shape=[jax.ShapeDtypeStruct((t, 2 * dh), BF)] * (2 * nq),
                compiler_params=_params(), cost_estimate=_cost(nq * 10e9, 13e6), name="attend",
            )(ids, *src)

        got = {}
        for ms in GROUPS:
            o = attend(ms)
            for i, m in enumerate(ms):
                for e in range(2):
                    v = m ^ e
                    got[v] = send(o[2 * i + e], lambda j, v=v: j ^ v) if v else o[2 * i + e]

        wo2 = wo.reshape(hh * dh, d)
        tn = 512
        o_spec = pl.BlockSpec((t, 2 * dh), lambda i, s: (0, 0))

        def w_spec(m):
            return pl.BlockSpec((2 * dh, tn), lambda i, s: (s[DEV + m], i))

        def project(ms, part=None):
            n = len(ms)
            col = pl.BlockSpec((t, tn), lambda i, s: (0, i))
            extra = [] if part is None else [part, x]
            return pl.pallas_call(
                _out_first if part is None else _out_last,
                grid_spec=pltpu.PrefetchScalarGridSpec(
                    num_scalar_prefetch=1, grid=(d // tn,),
                    in_specs=[o_spec] * n + [w_spec(m) for m in ms] + [col] * len(extra),
                    out_specs=col),
                out_shape=jax.ShapeDtypeStruct((t, d), F32 if part is None else BF),
                compiler_params=_params(), cost_estimate=_cost(n * 2 * t * 2 * dh * d * 1.3, n * 4.2e6 + 8e6),
                name="project",
            )(ids, *[got[m] for m in ms], *[wo2] * n, *extra)

        part = project((6, 7, 1, 0))
        return project((2, 3, 4, 5), part)

    return jax.shard_map(local, mesh=mesh,
                         in_specs=(rows, P(None), P(None, None, None, None), P(None, None, None)),
                         out_specs=rows, check_vma=False)
```

```python
import functools

import jax
import jax.numpy as jnp
from jax import lax
from jax.experimental import pallas as pl
from jax.experimental.pallas import tpu as pltpu
from jax.sharding import PartitionSpec as P


BF = jnp.bfloat16
F32 = jnp.float32
VMEM_LIMIT = 62 << 20
COST = 0.05
GROUPS = ((6, 0), (2, 4))
ME, B_TILE, B_HEADS, OWN_TILE, OWN_HEADS, SRC, DEV = 0, 1, 2, 6, 7, 11, 19


def _norm(x_ref, g_ref, xn, base):
    rb = 64

    def body(i, c):
        r = pl.ds(pl.multiple_of(i * rb, rb), rb)
        xf = x_ref[r, :].astype(F32)
        ms = jnp.mean(xf * xf, axis=-1, keepdims=True)
        xn[pl.ds(pl.multiple_of(base + i * rb, rb), rb), :] = (xf * lax.rsqrt(ms + 1e-5) * g_ref[...]).astype(BF)
        return c

    lax.fori_loop(0, x_ref.shape[0] // rb, body, 0)


def _rope_store(a, cos, sin, is_v, o_ref):
    half = a.shape[-1] // 2
    x1, x2 = a[:, :half], a[:, half:]
    c = jnp.where(is_v, 1.0, cos)
    s = jnp.where(is_v, 0.0, sin)
    o_ref[:, :half] = (x1 * c - x2 * s).astype(BF)
    o_ref[:, half:] = (x2 * c + x1 * s).astype(BF)


def _qkv_tiled(nrow, emit_w, heads_at, ids, *refs):
    xs = refs[:nrow]
    g_ref, w_ref, cos_ref, sin_ref, s_ref, c_ref = refs[nrow:nrow + 6]
    wr_ref = refs[nrow + 6] if emit_w else None
    xn, acc, wa, wb = refs[nrow + 6 + emit_w:]
    i = pl.program_id(0)
    bd, t = w_ref.shape[0], xs[0].shape[0]
    nd = xs[0].shape[1] // bd
    c, d = (i + nd - 1) // nd - 1, lax.rem(i + nd - 1, nd)

    def lay(dst):
        dst[...] = jnp.swapaxes(w_ref[:, 0], 0, 1)

    def use(src):
        ws = [src[ids[heads_at + j]] for j in range(4)]
        if emit_w:
            for j in range(4):
                wr_ref[0, j] = ws[j]
        xb = xn[:, pl.ds(pl.multiple_of(d * bd, bd), bd)]
        acc[...] += jnp.dot(xb, jnp.concatenate(ws, axis=1), preferred_element_type=F32)

    @pl.when(i == 0)
    def _():
        for b in range(nrow):
            _norm(xs[b], g_ref, xn, b * t)
        lay(wa)

    @pl.when((i > 0) & (d == 0))
    def _():
        acc[...] = jnp.zeros_like(acc)

    @pl.when(lax.rem(i, 2) == 1)
    def _():
        lay(wb)
        use(wa)

    @pl.when((lax.rem(i, 2) == 0) & (i > 0))
    def _():
        lay(wa)
        use(wb)

    @pl.when((i > 0) & (d == nd - 1))
    def _():
        for b in range(nrow):
            r = slice(b * t, (b + 1) * t)
            cos, sin = cos_ref[r], sin_ref[r]
            for j in range(4):
                o = s_ref if j < 2 else c_ref
                o = o.at[b, 0, j % 2] if nrow > 1 else o.at[0, j % 2]
                _rope_store(acc[r, j * 256:(j + 1) * 256], cos, sin, c == 2, o)


def _qkv_next(x_ref, g_ref, w_ref, cos_ref, sin_ref, s_ref, c_ref, xn):
    c, j = pl.program_id(0), pl.program_id(1)

    @pl.when((c == 0) & (j == 0))
    def _():
        _norm(x_ref, g_ref, xn, 0)

    def emit(o_ref):
        cos, sin = cos_ref[...], sin_ref[...]
        w = jnp.concatenate([w_ref[0, 0], w_ref[0, 1]], axis=1)
        a = jnp.dot(xn[...], w, preferred_element_type=F32)
        for h in range(2):
            _rope_store(a[:, h * 256:(h + 1) * 256], cos, sin, c == 2, o_ref.at[0, h])

    @pl.when(j == 0)
    def _():
        emit(s_ref)

    @pl.when(j == 1)
    def _():
        emit(c_ref)


def _attend(masks, ids, l_ref, rp_ref, rs0, rs1, rc0, rc1, *refs):
    nq = len(masks)
    outs = refs[:2 * nq]
    qkv, m_s, l_s, acc, sem = refs[2 * nq:]
    src = [l_ref.at[0], l_ref.at[1], rp_ref.at[0], rp_ref.at[1], rs0, rs1, rc0, rc1]
    t, dh = rs0.shape[2:]
    me = ids[ME]
    chips = [(me ^ m) // 2 for m in masks]
    last = functools.reduce(jnp.maximum, chips)

    def kv_copy(n, b):
        rows = pl.ds(pl.multiple_of(b * t, t), t)
        return pltpu.make_async_copy(src[n].at[pl.ds(1, 2)], qkv.at[pl.ds(1, 2), :, rows, :], sem.at[0, b])

    def q_copy(n, b):
        rows = pl.ds(pl.multiple_of(b * t, t), t)
        return pltpu.make_async_copy(src[n].at[0], qkv.at[0, :, rows, :], sem.at[1, b])

    for n in range(8):
        b = ids[SRC + n]
        want = functools.reduce(jnp.logical_or, [b // 2 == cc for cc in chips])

        @pl.when(want)
        def _():
            q_copy(n, b).start()

        @pl.when(b // 2 <= last)
        def _():
            kv_copy(n, b).start()

    k2 = (dh ** -0.5) * 1.4426950408889634

    k = me % 2

    def chip_rows(i, carry):
        cc = jnp.where(i == 0, chips[0], chips[1])
        q0 = pl.multiple_of(cc * 2 * t, 2 * t)
        for b in range(2):
            q_copy(0, 2 * cc + b).wait()
        m_s[...] = jnp.full_like(m_s, -jnp.inf)
        l_s[...] = jnp.zeros_like(l_s)
        acc[...] = jnp.zeros_like(acc)

        def kv_wait(j):
            @pl.when(i == 0)
            def _():
                for b in range(2):
                    kv_copy(0, 2 * j + b).wait()

        def tile(base, r0, nr, w, masked):
            rs = slice(r0, r0 + nr)
            ss = []
            for h in range(2):
                s = lax.dot_general(qkv[0, h, pl.ds(q0 + r0, nr), :], qkv[1, h, pl.ds(base, w), :],
                                    (((1,), (1,)), ((), ())), preferred_element_type=F32)
                if masked:
                    row = lax.broadcasted_iota(jnp.int32, (nr, w), 0)
                    col = lax.broadcasted_iota(jnp.int32, (nr, w), 1)
                    s = jnp.where(row >= col, s, -jnp.inf)
                ss.append(s)
            for h in range(2):
                ch = [ss[h][:, q * 128:(q + 1) * 128] for q in range(w // 128)]
                m_old = m_s[h, rs]
                m_new = jnp.maximum(m_old, jnp.max(functools.reduce(jnp.maximum, ch), axis=-1, keepdims=True))
                alpha = jnp.exp2((m_old - m_new) * k2)
                m_s[h, rs] = m_new
                mk = m_new * k2
                ps = [jnp.exp2(v * k2 - mk) for v in ch]
                l_s[h, rs] = l_s[h, rs] * alpha + functools.reduce(jnp.add, ps)
                p = jnp.concatenate([v.astype(BF) for v in ps], axis=1)
                pv = jnp.dot(p, qkv[2, h, pl.ds(base, w), :], preferred_element_type=F32)
                for q in range(dh // 128):
                    sl = slice(q * 128, (q + 1) * 128)
                    acc[h, rs, sl] = acc[h, rs, sl] * alpha + pv[:, sl]

        def body(j, carry):
            kv_wait(j)
            tile(pl.multiple_of(j * 2 * t, 2 * t), 0, 2 * t, 2 * t, False)
            return carry

        lax.fori_loop(0, cc, body, 0)
        kv_wait(cc)
        tile(q0, 0, t, t, True)
        tile(q0, t, t, t, False)
        tile(pl.multiple_of(q0 + t, t), t, t, t, True)

        @pl.when(i == 0)
        def _():
            def drain(j, carry):
                kv_wait(j)
                return carry

            lax.fori_loop(cc + 1, last + 1, drain, 0)

        for o in range(2):
            rs = pl.ds(pl.multiple_of((k if o == 0 else 1 - k) * t, t), t)
            for h in range(2):
                l = jnp.sum(l_s[h, rs, :], axis=-1, keepdims=True)
                v = (acc[h, rs, :] / l).astype(BF)
                for n in range(nq):
                    @pl.when(i == n)
                    def _(n=n):
                        outs[2 * n + o][:, h * dh:(h + 1) * dh] = v
        return carry

    lax.fori_loop(0, nq, chip_rows, 0)


def _out_first(ids, *refs):
    n = (len(refs) - 1) // 2
    o = jnp.concatenate([r[...] for r in refs[:n]], axis=1)
    w = jnp.concatenate([r[...] for r in refs[n:2 * n]], axis=0)
    refs[-1][...] = jnp.dot(o, w, preferred_element_type=F32)


def _out_last(ids, *refs):
    n = (len(refs) - 3) // 2
    o = jnp.concatenate([r[...] for r in refs[:n]], axis=1)
    w = jnp.concatenate([r[...] for r in refs[n:2 * n]], axis=0)
    part, x, out = refs[2 * n], refs[2 * n + 1], refs[-1]
    a = part[...] + jnp.dot(o, w, preferred_element_type=F32)
    out[...] = (x[...].astype(F32) + a).astype(BF)


def _params(**kw):
    return pltpu.CompilerParams(vmem_limit_bytes=VMEM_LIMIT, **kw)


def _cost(flops, nbytes):
    return pl.CostEstimate(flops=int(flops * COST), bytes_accessed=int(nbytes * COST), transcendentals=0)


def solution(mesh):
    rows = P(("data", "seq"), None)

    def local(x, g, wqkv, wo):
        t, d = x.shape
        _, _, hh, dh = wqkv.shape
        me = lax.axis_index("seq").astype(jnp.int32)
        k = me % 2
        kf, yf = 2 << k, 4 >> k

        def send(a, f):
            return lax.ppermute(a, "seq", [(i, f(i)) for i in range(8)])

        def to_a(i):
            return i ^ (2 << (i & 1))

        def to_same(i):
            return i ^ (4 >> (i & 1))

        def to_cross(i):
            return to_same(i) ^ 1

        inv = 10000.0 ** (-jnp.arange(dh // 2, dtype=F32) * 2.0 / dh)

        def tables(b):
            pos = (b[:, None] * t + jnp.arange(t)[None, :]).reshape(-1).astype(F32)
            ang = pos[:, None] * inv[None, :]
            return jnp.cos(ang), jnp.sin(ang)

        chip, a_id, so, po = me // 2, me ^ kf, me ^ yf, me ^ 1
        xo = po ^ kf

        def heads(ch):
            off = (ch % 2) * 4
            return [ch // 2, off + 2 * k, off + 2 * k + 1, off + 2 - 2 * k, off + 3 - 2 * k]

        ids = jnp.stack([me] + heads(so // 2) + heads(chip)
                        + [me, a_id, po, po ^ yf, so, me ^ 6, xo, me ^ 7]
                        + [me ^ m for m in range(8)]).astype(jnp.int32)
        cos, sin = tables(jnp.stack([me, a_id]))
        g2 = g[None, :]

        xa = send(x, to_a)

        half = jax.ShapeDtypeStruct((3, 2, t, dh), BF)
        both = jax.ShapeDtypeStruct((2, 3, 2, t, dh), BF)
        bd = 1024
        row_spec = pl.BlockSpec((t, d), lambda c, i: (0, 0), pipeline_mode=pl.Buffered(1))
        g_spec = pl.BlockSpec((1, d), lambda c, i: (0, 0))
        half_spec = pl.BlockSpec((1, 2, t, dh), lambda c, i: (c, 0, 0, 0))
        flops = 2 * t * d * 12 * dh

        def tab_spec(b):
            return pl.BlockSpec((t, dh // 2), lambda c, i: (b, 0))

        nd = d // bd
        steps = 3 * nd

        def tile_spec(at):
            def index(i, s):
                j = jnp.minimum(i, steps - 1)
                return lax.rem(j, nd), j // nd, s[at], 0

            return pl.BlockSpec((bd, 1, 8, dh), index)

        def prev(i):
            j = jnp.maximum(i - 1, 0)
            return j // nd, lax.rem(j, nd)

        rows1 = pl.BlockSpec((t, d), lambda i, s: (0, 0), pipeline_mode=pl.Buffered(1))
        g1 = pl.BlockSpec((1, d), lambda i, s: (0, 0))

        def tab1(n):
            return pl.BlockSpec((n * t, dh // 2), lambda i, s: (0, 0))

        half1 = pl.BlockSpec((1, 2, t, dh), lambda i, s: (prev(i)[0], 0, 0, 0))
        both1 = pl.BlockSpec((2, 1, 2, t, dh), lambda i, s: (0, prev(i)[0], 0, 0, 0))
        wr1 = pl.BlockSpec((1, 4, bd, dh), lambda i, s: (prev(i)[0], 0, prev(i)[1], 0))

        def tiled_scratch(n):
            return [pltpu.VMEM((n * t, d), BF), pltpu.VMEM((n * t, 4 * dh), F32),
                    pltpu.VMEM((8, bd, dh), BF), pltpu.VMEM((8, bd, dh), BF)]

        b_same, b_cross, w_b = pl.pallas_call(
            functools.partial(_qkv_tiled, 1, True, B_HEADS),
            grid_spec=pltpu.PrefetchScalarGridSpec(
                num_scalar_prefetch=1, grid=(steps + 1,),
                in_specs=[rows1, g1, tile_spec(B_TILE), tab1(1), tab1(1)],
                out_specs=[half1, half1, wr1],
                scratch_shapes=tiled_scratch(1)),
            out_shape=[half, half, jax.ShapeDtypeStruct((3, 4, d, dh), BF)],
            compiler_params=_params(), cost_estimate=_cost(flops * 2.5, 80e6), name="qkv_first",
        )(ids, x, g2, wqkv, cos, sin)
        rs_own, rc_own = send(b_same, to_same), send(b_cross, to_cross)
        a_same, a_cross = pl.pallas_call(
            _qkv_next,
            grid=(3, 2),
            in_specs=[row_spec, g_spec, pl.BlockSpec((1, 2, d, dh), lambda c, i: (c, i, 0, 0)),
                      tab_spec(1), tab_spec(1)],
            out_specs=[half_spec, half_spec],
            out_shape=[half, half],
            scratch_shapes=[pltpu.VMEM((t, d), BF)],
            compiler_params=_params(), cost_estimate=_cost(flops * 1.4, 35e6), name="qkv_next",
        )(xa, g2, w_b, cos, sin)
        rs_a, rc_a = send(a_same, to_same), send(a_cross, to_cross)
        loc, par = pl.pallas_call(
            functools.partial(_qkv_tiled, 2, False, OWN_HEADS),
            grid_spec=pltpu.PrefetchScalarGridSpec(
                num_scalar_prefetch=1, grid=(steps + 1,),
                in_specs=[rows1, rows1, g1, tile_spec(OWN_TILE), tab1(2), tab1(2)],
                out_specs=[both1, both1],
                scratch_shapes=tiled_scratch(2)),
            out_shape=[both, both],
            compiler_params=_params(), cost_estimate=_cost(flops * 2.8, 60e6), name="qkv_own",
        )(ids, x, xa, g2, wqkv, cos, sin)
        rpar = send(par, lambda i: i ^ 1)
        src = [loc, rpar, rs_own, rs_a, rc_own, rc_a]

        def attend(ms):
            nq = len(ms)
            anyspec = pl.BlockSpec(memory_space=pl.ANY)
            return pl.pallas_call(
                functools.partial(_attend, ms),
                grid_spec=pltpu.PrefetchScalarGridSpec(
                    num_scalar_prefetch=1, grid=(1,),
                    in_specs=[anyspec] * 6,
                    out_specs=[pl.BlockSpec((t, 2 * dh), lambda i, s: (0, 0))] * (2 * nq),
                    scratch_shapes=[pltpu.VMEM((3, 2, 8 * t, dh), BF),
                                    pltpu.VMEM((2, 2 * t, 128), F32), pltpu.VMEM((2, 2 * t, 128), F32),
                                    pltpu.VMEM((2, 2 * t, dh), F32), pltpu.SemaphoreType.DMA((2, 8))]),
                out_shape=[jax.ShapeDtypeStruct((t, 2 * dh), BF)] * (2 * nq),
                compiler_params=_params(), cost_estimate=_cost(nq * 10e9, 13e6), name="attend",
            )(ids, *src)

        got = {}
        for ms in GROUPS:
            o = attend(ms)
            for i, m in enumerate(ms):
                for e in range(2):
                    v = m ^ e
                    got[v] = send(o[2 * i + e], lambda j, v=v: j ^ v) if v else o[2 * i + e]

        wo2 = wo.reshape(hh * dh, d)
        tn = 512
        o_spec = pl.BlockSpec((t, 2 * dh), lambda i, s: (0, 0))

        def w_spec(m):
            return pl.BlockSpec((2 * dh, tn), lambda i, s: (s[DEV + m], i))

        def project(ms, part=None):
            n = len(ms)
            col = pl.BlockSpec((t, tn), lambda i, s: (0, i))
            extra = [] if part is None else [part, x]
            return pl.pallas_call(
                _out_first if part is None else _out_last,
                grid_spec=pltpu.PrefetchScalarGridSpec(
                    num_scalar_prefetch=1, grid=(d // tn,),
                    in_specs=[o_spec] * n + [w_spec(m) for m in ms] + [col] * len(extra),
                    out_specs=col),
                out_shape=jax.ShapeDtypeStruct((t, d), F32 if part is None else BF),
                compiler_params=_params(), cost_estimate=_cost(n * 2 * t * 2 * dh * d * 1.3, n * 4.2e6 + 8e6),
                name="project",
            )(ids, *[got[m] for m in ms], *[wo2] * n, *extra)

        part = project((6, 7, 1, 0))
        return project((2, 3, 4, 5), part)

    return jax.shard_map(local, mesh=mesh,
                         in_specs=(rows, P(None), P(None, None, None, None), P(None, None, None)),
                         out_specs=rows, check_vma=False)
```

```python
import functools

import jax
import jax.numpy as jnp
from jax import lax
from jax.experimental import pallas as pl
from jax.experimental.pallas import tpu as pltpu
from jax.sharding import PartitionSpec as P


BF = jnp.bfloat16
F32 = jnp.float32
VMEM_LIMIT = 62 << 20
COST = 0.05
GROUPS = ((2, 4), (6, 0))
ME, B_TILE, B_PART, OWN_TILE, OWN_PART, SRC, DEV = 0, 1, 2, 3, 4, 5, 13


def _norm(x_ref, g_ref, xn, base):
    rb = 16

    def body(i, c):
        r = pl.ds(pl.multiple_of(i * rb, rb), rb)
        xf = x_ref[r, :].astype(F32)
        ms = jnp.mean(xf * xf, axis=-1, keepdims=True)
        xn[pl.ds(pl.multiple_of(base + i * rb, rb), rb), :] = (xf * lax.rsqrt(ms + 1e-5) * g_ref[...]).astype(BF)
        return c

    lax.fori_loop(0, x_ref.shape[0] // rb, body, 0, unroll=2)


def _norm_rows(x_ref, g_ref, o_ref):
    _norm(x_ref, g_ref, o_ref, 0)


def _emit_heads(acc, cos, sin, is_v, outs):
    @pl.when(is_v)
    def _():
        for j, o in enumerate(outs):
            o[...] = acc[:, j * 256:(j + 1) * 256].astype(BF)

    @pl.when(jnp.logical_not(is_v))
    def _():
        cs, sn = cos[...], sin[...]
        for j, o in enumerate(outs):
            x1, x2 = acc[:, j * 256:j * 256 + 128], acc[:, j * 256 + 128:(j + 1) * 256]
            o[:, :128] = (x1 * cs - x2 * sn).astype(BF)
            o[:, 128:] = (x2 * cs + x1 * sn).astype(BF)


def _lay(w_ref, wt, at):
    bd, n = w_ref.shape[0], wt.shape[1]
    for p in range(8 * 256 // n):
        @pl.when(at == p)
        def _():
            wt[...] = w_ref[:, 0].reshape(bd, 8 * 256)[:, p * n:(p + 1) * n]


def _qkv_first(ids, x_ref, g_ref, w_ref, cos_ref, sin_ref, s_ref, c_ref, wr_ref, xn, acc):
    c, d = pl.program_id(0), pl.program_id(1)
    bd = w_ref.shape[0]

    @pl.when((c == 0) & (d == 0))
    def _():
        _norm(x_ref, g_ref, xn, 0)

    @pl.when(d == 0)
    def _():
        acc[...] = jnp.zeros_like(acc)

    _lay(w_ref, wr_ref.at[0], ids[B_PART])
    xb = xn[:, pl.ds(pl.multiple_of(d * bd, bd), bd)]
    acc[...] += jnp.dot(xb, wr_ref[0], preferred_element_type=F32)

    @pl.when(d == pl.num_programs(1) - 1)
    def _():
        k = ids[ME] % 2
        for o, kk in ((s_ref, k), (c_ref, 1 - k)):
            pair = acc.at[:, pl.ds(pl.multiple_of(kk * 512, 512), 512)]
            _emit_heads(pair, cos_ref, sin_ref, c == 2, [o.at[0, h] for h in range(2)])


def _qkv_own(ids, x0, x1, x2, x3, w_ref, tab_ref, ptab_ref, o_ref, xs, acc, wt, sem):
    c, d = pl.program_id(0), pl.program_id(1)
    nd = pl.num_programs(1)
    bd, t = w_ref.shape[0], x0.shape[0]

    def copy(b, k):
        cols = pl.ds(pl.multiple_of(k * bd, bd), bd)
        return pltpu.make_async_copy((x0, x1, x2, x3)[b].at[:, cols], xs.at[pl.ds(b * t, t), cols], sem.at[k, b])

    @pl.when((c == 0) & (d == 0))
    def _():
        for k in range(x0.shape[1] // bd):
            for b in range(4):
                copy(b, k).start()

    @pl.when(d == 0)
    def _():
        acc[...] = jnp.zeros_like(acc)

    @pl.when(c == 0)
    def _():
        for b in range(4):
            copy(b, d).wait()

    _lay(w_ref, wt, ids[OWN_PART])
    cols = pl.ds(pl.multiple_of(d * bd, bd), bd)
    for h in range(2):
        for m in range(2):
            r = slice(m * 2 * t, (m + 1) * 2 * t)
            acc[r, h * 256:(h + 1) * 256] += jnp.dot(xs[r, cols], wt[:, h * 256:(h + 1) * 256],
                                                     preferred_element_type=F32)

    @pl.when(d == nd - 1)
    def _():
        for b in range(4):
            r = pl.ds(b * t, t)
            tb = (tab_ref, ptab_ref)[b % 2]
            tr = pl.ds((b // 2) * t, t)
            _emit_heads(acc.at[r], tb.at[0, tr], tb.at[1, tr], c == 2, [o_ref.at[b, 0, h] for h in range(2)])


def _qkv_next(ids, xn, w_ref, cos_ref, sin_ref, s_ref, c_ref, acc):
    c, j = pl.program_id(0), pl.program_id(1)

    acc[...] = jnp.dot(xn[...], w_ref[0], preferred_element_type=F32)
    for n, o_ref in enumerate((s_ref, c_ref)):
        @pl.when(j == n)
        def _():
            _emit_heads(acc, cos_ref, sin_ref, c == 2, [o_ref.at[0, h] for h in range(2)])


def _attend(masks, ids, l_ref, rs0, rs1, rc0, rc1, *refs):
    nq = len(masks)
    outs = refs[:2 * nq]
    qkv, m_s, l_s, acc, sem = refs[2 * nq:]
    src = [l_ref.at[b] for b in range(4)] + [rs0, rs1, rc0, rc1]
    t, dh = rs0.shape[2:]
    me = ids[ME]
    chips = [(me ^ m) // 2 for m in masks]
    last = functools.reduce(jnp.maximum, chips)

    def kv_copy(n, b):
        rows = pl.ds(pl.multiple_of(b * t, t), t)
        return pltpu.make_async_copy(src[n].at[pl.ds(1, 2)], qkv.at[pl.ds(1, 2), :, rows, :], sem.at[0, b])

    def q_copy(n, b):
        rows = pl.ds(pl.multiple_of(b * t, t), t)
        return pltpu.make_async_copy(src[n].at[0], qkv.at[0, :, rows, :], sem.at[1, b])

    for n in range(8):
        b = ids[SRC + n]
        want = functools.reduce(jnp.logical_or, [b // 2 == cc for cc in chips])

        @pl.when(want)
        def _():
            q_copy(n, b).start()

        @pl.when(b // 2 <= last)
        def _():
            kv_copy(n, b).start()

    k2 = (dh ** -0.5) * 1.4426950408889634

    k = me % 2

    def chip_rows(i, carry):
        cc = jnp.where(i == 0, chips[0], chips[1])
        q0 = pl.multiple_of(cc * 2 * t, 2 * t)
        for b in range(2):
            q_copy(0, 2 * cc + b).wait()
        m_s[...] = jnp.full_like(m_s, -jnp.inf)
        l_s[...] = jnp.zeros_like(l_s)
        acc[...] = jnp.zeros_like(acc)

        def kv_wait(j):
            @pl.when(i == 0)
            def _():
                for b in range(2):
                    kv_copy(0, 2 * j + b).wait()

        def tile(base, r0, nr, w, masked):
            rs = slice(r0, r0 + nr)
            ss = []
            for h in range(2):
                s = lax.dot_general(qkv[0, h, pl.ds(q0 + r0, nr), :], qkv[1, h, pl.ds(base, w), :],
                                    (((1,), (1,)), ((), ())), preferred_element_type=F32)
                if masked:
                    row = lax.broadcasted_iota(jnp.int32, (nr, w), 0)
                    col = lax.broadcasted_iota(jnp.int32, (nr, w), 1)
                    s = jnp.where(row >= col, s, -jnp.inf)
                ss.append(s)
            for h in range(2):
                ch = [ss[h][:, q * 128:(q + 1) * 128] for q in range(w // 128)]
                m_old = m_s[h, rs]
                m_new = jnp.maximum(m_old, jnp.max(functools.reduce(jnp.maximum, ch), axis=-1, keepdims=True))
                alpha = jnp.exp2((m_old - m_new) * k2)
                m_s[h, rs] = m_new
                mk = m_new * k2
                ps = [jnp.exp2(v * k2 - mk) for v in ch]
                l_s[h, rs] = l_s[h, rs] * alpha + functools.reduce(jnp.add, ps)
                p = jnp.concatenate([v.astype(BF) for v in ps], axis=1)
                pv = jnp.dot(p, qkv[2, h, pl.ds(base, w), :], preferred_element_type=F32)
                for q in range(dh // 128):
                    sl = slice(q * 128, (q + 1) * 128)
                    acc[h, rs, sl] = acc[h, rs, sl] * alpha + pv[:, sl]

        def body(j, carry):
            kv_wait(j)
            tile(pl.multiple_of(j * 2 * t, 2 * t), 0, 2 * t, 2 * t, False)
            return carry

        lax.fori_loop(0, cc, body, 0)
        kv_wait(cc)
        tile(q0, 0, t, t, True)
        tile(q0, t, t, t, False)
        tile(pl.multiple_of(q0 + t, t), t, t, t, True)

        @pl.when(i == 0)
        def _():
            def drain(j, carry):
                kv_wait(j)
                return carry

            lax.fori_loop(cc + 1, last + 1, drain, 0)

        for o in range(2):
            rs = pl.ds(pl.multiple_of((k if o == 0 else 1 - k) * t, t), t)
            for h in range(2):
                l = jnp.sum(l_s[h, rs, :], axis=-1, keepdims=True)
                v = (acc[h, rs, :] / l).astype(BF)
                for n in range(nq):
                    @pl.when(i == n)
                    def _(n=n):
                        outs[2 * n + o][:, h * dh:(h + 1) * dh] = v
        return carry

    lax.fori_loop(0, nq, chip_rows, 0)


def _out_first(ids, *refs):
    n = (len(refs) - 1) // 2
    o = jnp.concatenate([r[...] for r in refs[:n]], axis=1)
    w = jnp.concatenate([r[...] for r in refs[n:2 * n]], axis=0)
    refs[-1][...] = jnp.dot(o, w, preferred_element_type=F32)


def _out_last(ids, *refs):
    n = (len(refs) - 3) // 2
    o = jnp.concatenate([r[...] for r in refs[:n]], axis=1)
    w = jnp.concatenate([r[...] for r in refs[n:2 * n]], axis=0)
    part, x, out = refs[2 * n], refs[2 * n + 1], refs[-1]
    a = part[...] + jnp.dot(o, w, preferred_element_type=F32)
    out[...] = (x[...].astype(F32) + a).astype(BF)


def _params(**kw):
    return pltpu.CompilerParams(vmem_limit_bytes=VMEM_LIMIT, **kw)


def _cost(flops, nbytes):
    return pl.CostEstimate(flops=int(flops * COST), bytes_accessed=int(nbytes * COST), transcendentals=0)


def solution(mesh):
    rows = P(("data", "seq"), None)

    def local(x, g, wqkv, wo):
        t, d = x.shape
        _, _, hh, dh = wqkv.shape
        me = lax.axis_index("seq").astype(jnp.int32)
        k = me % 2
        kf, yf = 2 << k, 4 >> k

        def send(a, f):
            return lax.ppermute(a, "seq", [(i, f(i)) for i in range(8)])

        def to_a(i):
            return i ^ (2 << (i & 1))

        def to_same(i):
            return i ^ (4 >> (i & 1))

        def to_cross(i):
            return to_same(i) ^ 1

        inv = 10000.0 ** (-jnp.arange(dh // 2, dtype=F32) * 2.0 / dh)

        def tables(b):
            pos = (b[:, None] * t + jnp.arange(t)[None, :]).reshape(-1).astype(F32)
            ang = pos[:, None] * inv[None, :]
            return jnp.stack([jnp.cos(ang), jnp.sin(ang)])

        a_id, so, po = me ^ kf, me ^ yf, me ^ 1
        xo = po ^ kf

        ids = jnp.stack([me, so // 4, (so // 2) % 2, me // 4, me % 4]
                        + [me, po, a_id, po ^ yf, so, me ^ 6, xo, me ^ 7]
                        + [me ^ m for m in range(8)]).astype(jnp.int32)
        tab = tables(jnp.stack([me, a_id]))
        g2 = g[None, :]

        xa = send(x, to_a)

        half = jax.ShapeDtypeStruct((3, 2, t, dh), BF)
        xn_shape = jax.ShapeDtypeStruct((t, d), BF)
        bd = 1024
        nd = d // bd
        flops = 2 * t * d * 12 * dh

        def partner(a):
            return send(a, lambda i: i ^ 1)

        def tile_spec(at):
            return pl.BlockSpec((bd, 1, 8, dh), lambda c, i, s: (i, c, s[at], 0))

        def tab_spec(n, b):
            return pl.BlockSpec((pl.Squeezed(), t, dh // 2), lambda *_: (n, b, 0))

        whole = pl.BlockSpec((t, d), lambda *_: (0, 0), pipeline_mode=pl.Buffered(1))
        anyspec = pl.BlockSpec(memory_space=pl.ANY)
        half2 = pl.BlockSpec((1, 2, t, dh), lambda c, *_: (c, 0, 0, 0))

        b_same, b_cross, w_b, xn_o = pl.pallas_call(
            _qkv_first,
            grid_spec=pltpu.PrefetchScalarGridSpec(
                num_scalar_prefetch=1, grid=(3, nd),
                in_specs=[whole, pl.BlockSpec((1, d), lambda *_: (0, 0)), tile_spec(B_TILE),
                          tab_spec(0, 0), tab_spec(1, 0)],
                out_specs=[half2, half2, pl.BlockSpec((1, bd, 4 * dh), lambda c, i, s: (c, i, 0)), whole],
                scratch_shapes=[pltpu.VMEM((t, 4 * dh), F32)]),
            out_shape=[half, half, jax.ShapeDtypeStruct((3, d, 4 * dh), BF), xn_shape],
            compiler_params=_params(), cost_estimate=_cost(flops * 2.5, 80e6), name="qkv_first",
        )(ids, x, g2, wqkv, tab, tab)
        rs_own, rc_own = send(b_same, to_same), send(b_cross, to_cross)
        xn_po, ptab = partner(xn_o), partner(tab)
        rb = 128
        xn_a = pl.pallas_call(
            _norm_rows, grid=(t // rb,),
            in_specs=[pl.BlockSpec((rb, d), lambda i: (i, 0)), pl.BlockSpec((1, d), lambda i: (0, 0))],
            out_specs=pl.BlockSpec((rb, d), lambda i: (i, 0)), out_shape=xn_shape,
            compiler_params=_params(), cost_estimate=_cost(2e9, 8e6), name="norm",
        )(xa, g2)
        xn_pa = partner(xn_a)
        a_same, a_cross = pl.pallas_call(
            _qkv_next,
            grid_spec=pltpu.PrefetchScalarGridSpec(
                num_scalar_prefetch=1, grid=(3, 2),
                in_specs=[whole, pl.BlockSpec((1, d, 2 * dh), lambda c, i, s: (c, 0, (i + s[ME]) % 2)),
                          tab_spec(0, 1), tab_spec(1, 1)],
                out_specs=[half2, half2],
                scratch_shapes=[pltpu.VMEM((t, 2 * dh), F32)]),
            out_shape=[half, half],
            compiler_params=_params(), cost_estimate=_cost(flops * 1.4, 35e6), name="qkv_next",
        )(ids, xn_a, w_b, tab, tab)
        rs_a, rc_a = send(a_same, to_same), send(a_cross, to_cross)
        both_tab = pl.BlockSpec((2, 2 * t, dh // 2), lambda *_: (0, 0, 0), pipeline_mode=pl.Buffered(1))
        loc = pl.pallas_call(
            _qkv_own,
            grid_spec=pltpu.PrefetchScalarGridSpec(
                num_scalar_prefetch=1, grid=(3, nd),
                in_specs=[anyspec] * 4 + [tile_spec(OWN_TILE), both_tab, both_tab],
                out_specs=pl.BlockSpec((4, 1, 2, t, dh), lambda c, i, s: (0, c, 0, 0, 0)),
                scratch_shapes=[pltpu.VMEM((4 * t, d), BF), pltpu.VMEM((4 * t, 2 * dh), F32),
                                pltpu.VMEM((bd, 2 * dh), BF), pltpu.SemaphoreType.DMA((nd, 4))]),
            out_shape=jax.ShapeDtypeStruct((4, 3, 2, t, dh), BF),
            compiler_params=_params(), cost_estimate=_cost(flops * 2.8, 60e6), name="qkv_own",
        )(ids, xn_o, xn_po, xn_a, xn_pa, wqkv, tab, ptab)
        src = [loc, rs_own, rs_a, rc_own, rc_a]

        def attend(ms):
            nq = len(ms)
            return pl.pallas_call(
                functools.partial(_attend, ms),
                grid_spec=pltpu.PrefetchScalarGridSpec(
                    num_scalar_prefetch=1, grid=(1,),
                    in_specs=[anyspec] * 5,
                    out_specs=[pl.BlockSpec((t, 2 * dh), lambda i, s: (0, 0))] * (2 * nq),
                    scratch_shapes=[pltpu.VMEM((3, 2, 8 * t, dh), BF),
                                    pltpu.VMEM((2, 2 * t, 128), F32), pltpu.VMEM((2, 2 * t, 128), F32),
                                    pltpu.VMEM((2, 2 * t, dh), F32), pltpu.SemaphoreType.DMA((2, 8))]),
                out_shape=[jax.ShapeDtypeStruct((t, 2 * dh), BF)] * (2 * nq),
                compiler_params=_params(), cost_estimate=_cost(nq * 10e9, 13e6), name="attend",
            )(ids, *src)

        got = {}
        for ms in GROUPS:
            o = attend(ms)
            for i, m in enumerate(ms):
                for e in range(2):
                    v = m ^ e
                    got[v] = send(o[2 * i + e], lambda j, v=v: j ^ v) if v else o[2 * i + e]

        wo2 = wo.reshape(hh * dh, d)
        tn = 1024
        o_spec = pl.BlockSpec((t, 2 * dh), lambda i, s: (0, 0))

        def w_spec(m):
            return pl.BlockSpec((2 * dh, tn), lambda i, s: (s[DEV + m], i))

        def project(ms, part=None):
            n = len(ms)
            col = pl.BlockSpec((t, tn), lambda i, s: (0, i))
            extra = [] if part is None else [part, x]
            return pl.pallas_call(
                _out_first if part is None else _out_last,
                grid_spec=pltpu.PrefetchScalarGridSpec(
                    num_scalar_prefetch=1, grid=(d // tn,),
                    in_specs=[o_spec] * n + [w_spec(m) for m in ms] + [col] * len(extra),
                    out_specs=col),
                out_shape=jax.ShapeDtypeStruct((t, d), F32 if part is None else BF),
                compiler_params=_params(), cost_estimate=_cost(n * 2 * t * 2 * dh * d * 1.3, n * 4.2e6 + 8e6),
                name="project",
            )(ids, *[got[m] for m in ms], *[wo2] * n, *extra)

        part = project((0, 1, 2, 3, 4, 5))
        return project((6, 7), part)

    return jax.shard_map(local, mesh=mesh,
                         in_specs=(rows, P(None), P(None, None, None, None), P(None, None, None)),
                         out_specs=rows, check_vma=False)
```

```python
import functools

import jax
import jax.numpy as jnp
from jax import lax
from jax.experimental import pallas as pl
from jax.experimental.pallas import tpu as pltpu
from jax.sharding import PartitionSpec as P


BF = jnp.bfloat16
F32 = jnp.float32
VMEM_LIMIT = 62 << 20
COST = 0.05
GROUPS = ((2, 4), (6, 0))
ME, B_HEAD, OWN_HEAD, SRC, DEV = 0, 1, 2, 3, 11


def _norm(x_ref, g_ref, xn, base):
    rb = 16

    def body(i, c):
        r = pl.ds(pl.multiple_of(i * rb, rb), rb)
        xf = x_ref[r, :].astype(F32)
        ms = jnp.mean(xf * xf, axis=-1, keepdims=True)
        xn[pl.ds(pl.multiple_of(base + i * rb, rb), rb), :] = (xf * lax.rsqrt(ms + 1e-5) * g_ref[...]).astype(BF)
        return c

    lax.fori_loop(0, x_ref.shape[0] // rb, body, 0, unroll=2)


def _norm_rows(x_ref, g_ref, o_ref):
    _norm(x_ref, g_ref, o_ref, 0)


def _emit_heads(acc, cos, sin, is_v, outs):
    @pl.when(is_v)
    def _():
        for j, o in enumerate(outs):
            o[...] = acc[:, j * 256:(j + 1) * 256].astype(BF)

    @pl.when(jnp.logical_not(is_v))
    def _():
        cs, sn = cos[...], sin[...]
        for j, o in enumerate(outs):
            x1, x2 = acc[:, j * 256:j * 256 + 128], acc[:, j * 256 + 128:(j + 1) * 256]
            o[:, :128] = (x1 * cs - x2 * sn).astype(BF)
            o[:, 128:] = (x2 * cs + x1 * sn).astype(BF)


def _stream(w_ref, buf, sem, head):
    c, d = pl.program_id(0), pl.program_id(1)
    nc, nd = pl.num_programs(0), pl.num_programs(1)
    _, bd, n, dh = buf.shape
    i = c * nd + d

    def copy(j):
        rows = pl.ds(pl.multiple_of(lax.rem(j, nd) * bd, bd), bd)
        heads = pl.ds(pl.multiple_of(head, n), n)
        return pltpu.make_async_copy(w_ref.at[rows, j // nd, heads, :], buf.at[j % 2], sem.at[j % 2])

    @pl.when(i == 0)
    def _():
        copy(0).start()

    @pl.when(i + 1 < nc * nd)
    def _():
        copy(i + 1).start()

    def take():
        copy(i).wait()
        return buf[i % 2].reshape(bd, n * dh)

    return take


def _qkv_first(ids, x_ref, g_ref, w_ref, cos_ref, sin_ref, s_ref, c_ref, wr_ref, xn, acc, buf, wsem):
    c, d = pl.program_id(0), pl.program_id(1)
    bd = buf.shape[1]
    take = _stream(w_ref, buf, wsem, ids[B_HEAD])

    @pl.when((c == 0) & (d == 0))
    def _():
        _norm(x_ref, g_ref, xn, 0)

    @pl.when(d == 0)
    def _():
        acc[...] = jnp.zeros_like(acc)

    wr_ref[0] = take()
    xb = xn[:, pl.ds(pl.multiple_of(d * bd, bd), bd)]
    acc[...] += jnp.dot(xb, wr_ref[0], preferred_element_type=F32)

    @pl.when(d == pl.num_programs(1) - 1)
    def _():
        k = ids[ME] % 2
        for o, kk in ((s_ref, k), (c_ref, 1 - k)):
            pair = acc.at[:, pl.ds(pl.multiple_of(kk * 512, 512), 512)]
            _emit_heads(pair, cos_ref, sin_ref, c == 2, [o.at[0, h] for h in range(2)])


def _qkv_own(ids, x0, x1, x2, x3, w_ref, tab_ref, ptab_ref, o_ref, xs, acc, wt, sem, buf, wsem):
    c, d = pl.program_id(0), pl.program_id(1)
    nd = pl.num_programs(1)
    bd, t = buf.shape[1], x0.shape[0]
    take = _stream(w_ref, buf, wsem, ids[OWN_HEAD])

    def copy(b, k):
        cols = pl.ds(pl.multiple_of(k * bd, bd), bd)
        return pltpu.make_async_copy((x0, x1, x2, x3)[b].at[:, cols], xs.at[pl.ds(b * t, t), cols], sem.at[k, b])

    @pl.when((c == 0) & (d == 0))
    def _():
        for k in range(x0.shape[1] // bd):
            for b in range(4):
                copy(b, k).start()

    @pl.when(d == 0)
    def _():
        acc[...] = jnp.zeros_like(acc)

    @pl.when(c == 0)
    def _():
        for b in range(4):
            copy(b, d).wait()

    wt[...] = take()
    cols = pl.ds(pl.multiple_of(d * bd, bd), bd)
    for h in range(2):
        for m in range(2):
            r = slice(m * 2 * t, (m + 1) * 2 * t)
            acc[r, h * 256:(h + 1) * 256] += jnp.dot(xs[r, cols], wt[:, h * 256:(h + 1) * 256],
                                                     preferred_element_type=F32)

    @pl.when(d == nd - 1)
    def _():
        for b in range(4):
            r = pl.ds(b * t, t)
            tb = (tab_ref, ptab_ref)[b % 2]
            tr = pl.ds((b // 2) * t, t)
            _emit_heads(acc.at[r], tb.at[0, tr], tb.at[1, tr], c == 2, [o_ref.at[b, 0, h] for h in range(2)])


def _qkv_next(ids, xn, w_ref, cos_ref, sin_ref, s_ref, c_ref, acc):
    c, j = pl.program_id(0), pl.program_id(1)

    acc[...] = jnp.dot(xn[...], w_ref[0], preferred_element_type=F32)
    for n, o_ref in enumerate((s_ref, c_ref)):
        @pl.when(j == n)
        def _():
            _emit_heads(acc, cos_ref, sin_ref, c == 2, [o_ref.at[0, h] for h in range(2)])


def _attend(masks, ids, l_ref, rs0, rs1, rc0, rc1, *refs):
    nq = len(masks)
    outs = refs[:2 * nq]
    qkv, m_s, l_s, acc, sem = refs[2 * nq:]
    src = [l_ref.at[b] for b in range(4)] + [rs0, rs1, rc0, rc1]
    t, dh = rs0.shape[2:]
    me = ids[ME]
    chips = [(me ^ m) // 2 for m in masks]
    last = functools.reduce(jnp.maximum, chips)

    def kv_copy(n, b):
        rows = pl.ds(pl.multiple_of(b * t, t), t)
        return pltpu.make_async_copy(src[n].at[pl.ds(1, 2)], qkv.at[pl.ds(1, 2), :, rows, :], sem.at[0, b])

    def q_copy(n, b):
        rows = pl.ds(pl.multiple_of(b * t, t), t)
        return pltpu.make_async_copy(src[n].at[0], qkv.at[0, :, rows, :], sem.at[1, b])

    for n in range(8):
        b = ids[SRC + n]
        want = functools.reduce(jnp.logical_or, [b // 2 == cc for cc in chips])

        @pl.when(want)
        def _():
            q_copy(n, b).start()

        @pl.when(b // 2 <= last)
        def _():
            kv_copy(n, b).start()

    k2 = (dh ** -0.5) * 1.4426950408889634

    k = me % 2

    def chip_rows(i, carry):
        cc = jnp.where(i == 0, chips[0], chips[1])
        q0 = pl.multiple_of(cc * 2 * t, 2 * t)
        for b in range(2):
            q_copy(0, 2 * cc + b).wait()
        m_s[...] = jnp.full_like(m_s, -jnp.inf)
        l_s[...] = jnp.zeros_like(l_s)
        acc[...] = jnp.zeros_like(acc)

        def kv_wait(j):
            @pl.when(i == 0)
            def _():
                for b in range(2):
                    kv_copy(0, 2 * j + b).wait()

        def tile(base, r0, nr, w, masked):
            rs = slice(r0, r0 + nr)
            ss = []
            for h in range(2):
                s = lax.dot_general(qkv[0, h, pl.ds(q0 + r0, nr), :], qkv[1, h, pl.ds(base, w), :],
                                    (((1,), (1,)), ((), ())), preferred_element_type=F32)
                if masked:
                    row = lax.broadcasted_iota(jnp.int32, (nr, w), 0)
                    col = lax.broadcasted_iota(jnp.int32, (nr, w), 1)
                    s = jnp.where(row >= col, s, -jnp.inf)
                ss.append(s)
            for h in range(2):
                ch = [ss[h][:, q * 128:(q + 1) * 128] for q in range(w // 128)]
                m_old = m_s[h, rs]
                m_new = jnp.maximum(m_old, jnp.max(functools.reduce(jnp.maximum, ch), axis=-1, keepdims=True))
                alpha = jnp.exp2((m_old - m_new) * k2)
                m_s[h, rs] = m_new
                mk = m_new * k2
                ps = [jnp.exp2(v * k2 - mk) for v in ch]
                l_s[h, rs] = l_s[h, rs] * alpha + functools.reduce(jnp.add, ps)
                p = jnp.concatenate([v.astype(BF) for v in ps], axis=1)
                pv = jnp.dot(p, qkv[2, h, pl.ds(base, w), :], preferred_element_type=F32)
                for q in range(dh // 128):
                    sl = slice(q * 128, (q + 1) * 128)
                    acc[h, rs, sl] = acc[h, rs, sl] * alpha + pv[:, sl]

        def body(j, carry):
            kv_wait(j)
            tile(pl.multiple_of(j * 2 * t, 2 * t), 0, 2 * t, 2 * t, False)
            return carry

        lax.fori_loop(0, cc, body, 0)
        kv_wait(cc)
        tile(q0, 0, t, t, True)
        tile(q0, t, t, t, False)
        tile(pl.multiple_of(q0 + t, t), t, t, t, True)

        @pl.when(i == 0)
        def _():
            def drain(j, carry):
                kv_wait(j)
                return carry

            lax.fori_loop(cc + 1, last + 1, drain, 0)

        for o in range(2):
            rs = pl.ds(pl.multiple_of((k if o == 0 else 1 - k) * t, t), t)
            for h in range(2):
                l = jnp.sum(l_s[h, rs, :], axis=-1, keepdims=True)
                v = (acc[h, rs, :] / l).astype(BF)
                for n in range(nq):
                    @pl.when(i == n)
                    def _(n=n):
                        outs[2 * n + o][:, h * dh:(h + 1) * dh] = v
        return carry

    lax.fori_loop(0, nq, chip_rows, 0)


def _out_first(ids, *refs):
    n = (len(refs) - 1) // 2
    o = jnp.concatenate([r[...] for r in refs[:n]], axis=1)
    w = jnp.concatenate([r[...] for r in refs[n:2 * n]], axis=0)
    refs[-1][...] = jnp.dot(o, w, preferred_element_type=F32)


def _out_last(ids, *refs):
    n = (len(refs) - 3) // 2
    o = jnp.concatenate([r[...] for r in refs[:n]], axis=1)
    w = jnp.concatenate([r[...] for r in refs[n:2 * n]], axis=0)
    part, x, out = refs[2 * n], refs[2 * n + 1], refs[-1]
    a = part[...] + jnp.dot(o, w, preferred_element_type=F32)
    out[...] = (x[...].astype(F32) + a).astype(BF)


def _params(**kw):
    return pltpu.CompilerParams(vmem_limit_bytes=VMEM_LIMIT, **kw)


def _cost(flops, nbytes):
    return pl.CostEstimate(flops=int(flops * COST), bytes_accessed=int(nbytes * COST), transcendentals=0)


def solution(mesh):
    rows = P(("data", "seq"), None)

    def local(x, g, wqkv, wo):
        t, d = x.shape
        _, _, hh, dh = wqkv.shape
        me = lax.axis_index("seq").astype(jnp.int32)
        k = me % 2
        kf, yf = 2 << k, 4 >> k

        def send(a, f):
            return lax.ppermute(a, "seq", [(i, f(i)) for i in range(8)])

        def to_a(i):
            return i ^ (2 << (i & 1))

        def to_same(i):
            return i ^ (4 >> (i & 1))

        def to_cross(i):
            return to_same(i) ^ 1

        inv = 10000.0 ** (-jnp.arange(dh // 2, dtype=F32) * 2.0 / dh)

        def tables(b):
            pos = (b[:, None] * t + jnp.arange(t)[None, :]).reshape(-1).astype(F32)
            ang = pos[:, None] * inv[None, :]
            return jnp.stack([jnp.cos(ang), jnp.sin(ang)])

        a_id, so, po = me ^ kf, me ^ yf, me ^ 1
        xo = po ^ kf

        ids = jnp.stack([me, so // 2 * 4, me * 2]
                        + [me, po, a_id, po ^ yf, so, me ^ 6, xo, me ^ 7]
                        + [me ^ m for m in range(8)]).astype(jnp.int32)
        tab = tables(jnp.stack([me, a_id]))
        g2 = g[None, :]

        xa = send(x, to_a)

        half = jax.ShapeDtypeStruct((3, 2, t, dh), BF)
        xn_shape = jax.ShapeDtypeStruct((t, d), BF)
        bd = 1024
        nd = d // bd
        flops = 2 * t * d * 12 * dh

        def partner(a):
            return send(a, lambda i: i ^ 1)

        def tiles(n):
            return [pltpu.VMEM((2, bd, n, dh), BF), pltpu.SemaphoreType.DMA((2,))]

        def tab_spec(n, b):
            return pl.BlockSpec((pl.Squeezed(), t, dh // 2), lambda *_: (n, b, 0))

        whole = pl.BlockSpec((t, d), lambda *_: (0, 0), pipeline_mode=pl.Buffered(1))
        anyspec = pl.BlockSpec(memory_space=pl.ANY)
        half2 = pl.BlockSpec((1, 2, t, dh), lambda c, *_: (c, 0, 0, 0))

        b_same, b_cross, w_b, xn_o = pl.pallas_call(
            _qkv_first,
            grid_spec=pltpu.PrefetchScalarGridSpec(
                num_scalar_prefetch=1, grid=(3, nd),
                in_specs=[whole, pl.BlockSpec((1, d), lambda *_: (0, 0)), anyspec,
                          tab_spec(0, 0), tab_spec(1, 0)],
                out_specs=[half2, half2, pl.BlockSpec((1, bd, 4 * dh), lambda c, i, s: (c, i, 0)), whole],
                scratch_shapes=[pltpu.VMEM((t, 4 * dh), F32)] + tiles(4)),
            out_shape=[half, half, jax.ShapeDtypeStruct((3, d, 4 * dh), BF), xn_shape],
            compiler_params=_params(), cost_estimate=_cost(flops * 2.5, 80e6), name="qkv_first",
        )(ids, x, g2, wqkv, tab, tab)
        rs_own, rc_own = send(b_same, to_same), send(b_cross, to_cross)
        xn_po, ptab = partner(xn_o), partner(tab)
        rb = 128
        xn_a = pl.pallas_call(
            _norm_rows, grid=(t // rb,),
            in_specs=[pl.BlockSpec((rb, d), lambda i: (i, 0)), pl.BlockSpec((1, d), lambda i: (0, 0))],
            out_specs=pl.BlockSpec((rb, d), lambda i: (i, 0)), out_shape=xn_shape,
            compiler_params=_params(), cost_estimate=_cost(2e9, 8e6), name="norm",
        )(xa, g2)
        xn_pa = partner(xn_a)
        a_same, a_cross = pl.pallas_call(
            _qkv_next,
            grid_spec=pltpu.PrefetchScalarGridSpec(
                num_scalar_prefetch=1, grid=(3, 2),
                in_specs=[whole, pl.BlockSpec((1, d, 2 * dh), lambda c, i, s: (c, 0, (i + s[ME]) % 2)),
                          tab_spec(0, 1), tab_spec(1, 1)],
                out_specs=[half2, half2],
                scratch_shapes=[pltpu.VMEM((t, 2 * dh), F32)]),
            out_shape=[half, half],
            compiler_params=_params(), cost_estimate=_cost(flops * 1.4, 35e6), name="qkv_next",
        )(ids, xn_a, w_b, tab, tab)
        rs_a, rc_a = send(a_same, to_same), send(a_cross, to_cross)
        both_tab = pl.BlockSpec((2, 2 * t, dh // 2), lambda *_: (0, 0, 0), pipeline_mode=pl.Buffered(1))
        loc = pl.pallas_call(
            _qkv_own,
            grid_spec=pltpu.PrefetchScalarGridSpec(
                num_scalar_prefetch=1, grid=(3, nd),
                in_specs=[anyspec] * 5 + [both_tab, both_tab],
                out_specs=pl.BlockSpec((4, 1, 2, t, dh), lambda c, i, s: (0, c, 0, 0, 0)),
                scratch_shapes=[pltpu.VMEM((4 * t, d), BF), pltpu.VMEM((4 * t, 2 * dh), F32),
                                pltpu.VMEM((bd, 2 * dh), BF), pltpu.SemaphoreType.DMA((nd, 4))]
                + tiles(2)),
            out_shape=jax.ShapeDtypeStruct((4, 3, 2, t, dh), BF),
            compiler_params=_params(), cost_estimate=_cost(flops * 2.8, 60e6), name="qkv_own",
        )(ids, xn_o, xn_po, xn_a, xn_pa, wqkv, tab, ptab)
        src = [loc, rs_own, rs_a, rc_own, rc_a]

        def attend(ms):
            nq = len(ms)
            return pl.pallas_call(
                functools.partial(_attend, ms),
                grid_spec=pltpu.PrefetchScalarGridSpec(
                    num_scalar_prefetch=1, grid=(1,),
                    in_specs=[anyspec] * 5,
                    out_specs=[pl.BlockSpec((t, 2 * dh), lambda i, s: (0, 0))] * (2 * nq),
                    scratch_shapes=[pltpu.VMEM((3, 2, 8 * t, dh), BF),
                                    pltpu.VMEM((2, 2 * t, 128), F32), pltpu.VMEM((2, 2 * t, 128), F32),
                                    pltpu.VMEM((2, 2 * t, dh), F32), pltpu.SemaphoreType.DMA((2, 8))]),
                out_shape=[jax.ShapeDtypeStruct((t, 2 * dh), BF)] * (2 * nq),
                compiler_params=_params(), cost_estimate=_cost(nq * 10e9, 13e6), name="attend",
            )(ids, *src)

        got = {}
        for ms in GROUPS:
            o = attend(ms)
            for i, m in enumerate(ms):
                for e in range(2):
                    v = m ^ e
                    got[v] = send(o[2 * i + e], lambda j, v=v: j ^ v) if v else o[2 * i + e]

        wo2 = wo.reshape(hh * dh, d)
        tn = 1024
        o_spec = pl.BlockSpec((t, 2 * dh), lambda i, s: (0, 0))

        def w_spec(m):
            return pl.BlockSpec((2 * dh, tn), lambda i, s: (s[DEV + m], i))

        def project(ms, part=None):
            n = len(ms)
            col = pl.BlockSpec((t, tn), lambda i, s: (0, i))
            extra = [] if part is None else [part, x]
            return pl.pallas_call(
                _out_first if part is None else _out_last,
                grid_spec=pltpu.PrefetchScalarGridSpec(
                    num_scalar_prefetch=1, grid=(d // tn,),
                    in_specs=[o_spec] * n + [w_spec(m) for m in ms] + [col] * len(extra),
                    out_specs=col),
                out_shape=jax.ShapeDtypeStruct((t, d), F32 if part is None else BF),
                compiler_params=_params(), cost_estimate=_cost(n * 2 * t * 2 * dh * d * 1.3, n * 4.2e6 + 8e6),
                name="project",
            )(ids, *[got[m] for m in ms], *[wo2] * n, *extra)

        part = project((0, 1, 2, 3, 4, 5))
        return project((6, 7), part)

    return jax.shard_map(local, mesh=mesh,
                         in_specs=(rows, P(None), P(None, None, None, None), P(None, None, None)),
                         out_specs=rows, check_vma=False)
```

```python
import functools

import jax
import jax.numpy as jnp
from jax import lax
from jax.experimental import pallas as pl
from jax.experimental.pallas import tpu as pltpu
from jax.sharding import PartitionSpec as P


BF = jnp.bfloat16
F32 = jnp.float32
VMEM_LIMIT = 62 << 20
PROJ_VMEM = 40 << 20
COST = 0.05
TN0, TN1 = 1024, 1024
GROUPS = ((2, 4), (6, 0))
ME, B_HEAD, OWN_HEAD, SRC, DEV = 0, 1, 2, 3, 11


def _norm(x_ref, g_ref, xn, base):
    rb = 16

    def body(i, c):
        r = pl.ds(pl.multiple_of(i * rb, rb), rb)
        xf = x_ref[r, :].astype(F32)
        ms = jnp.mean(xf * xf, axis=-1, keepdims=True)
        xn[pl.ds(pl.multiple_of(base + i * rb, rb), rb), :] = (xf * lax.rsqrt(ms + 1e-5) * g_ref[...]).astype(BF)
        return c

    lax.fori_loop(0, x_ref.shape[0] // rb, body, 0, unroll=2)


def _norm_rows(x_ref, g_ref, o_ref):
    _norm(x_ref, g_ref, o_ref, 0)


def _emit_heads(acc, cos, sin, is_v, outs):
    @pl.when(is_v)
    def _():
        for j, o in enumerate(outs):
            o[...] = acc[:, j * 256:(j + 1) * 256].astype(BF)

    @pl.when(jnp.logical_not(is_v))
    def _():
        cs, sn = cos[...], sin[...]
        for j, o in enumerate(outs):
            x1, x2 = acc[:, j * 256:j * 256 + 128], acc[:, j * 256 + 128:(j + 1) * 256]
            o[:, :128] = (x1 * cs - x2 * sn).astype(BF)
            o[:, 128:] = (x2 * cs + x1 * sn).astype(BF)


def _stream(w_ref, buf, sem, head):
    c, d = pl.program_id(0), pl.program_id(1)
    nc, nd = pl.num_programs(0), pl.num_programs(1)
    _, bd, n, dh = buf.shape
    i = c * nd + d

    def copy(j):
        rows = pl.ds(pl.multiple_of(lax.rem(j, nd) * bd, bd), bd)
        heads = pl.ds(pl.multiple_of(head, n), n)
        return pltpu.make_async_copy(w_ref.at[rows, j // nd, heads, :], buf.at[j % 2], sem.at[j % 2])

    @pl.when(i == 0)
    def _():
        copy(0).start()

    @pl.when(i + 1 < nc * nd)
    def _():
        copy(i + 1).start()

    def take():
        copy(i).wait()
        return buf[i % 2].reshape(bd, n * dh)

    return take


def _qkv_first(ids, x_ref, g_ref, w_ref, cos_ref, sin_ref, s_ref, c_ref, wr_ref, xn, acc, buf, wsem):
    c, d = pl.program_id(0), pl.program_id(1)
    bd = buf.shape[1]
    take = _stream(w_ref, buf, wsem, ids[B_HEAD])

    @pl.when((c == 0) & (d == 0))
    def _():
        _norm(x_ref, g_ref, xn, 0)

    @pl.when(d == 0)
    def _():
        acc[...] = jnp.zeros_like(acc)

    wr_ref[0] = take()
    xb = xn[:, pl.ds(pl.multiple_of(d * bd, bd), bd)]
    acc[...] += jnp.dot(xb, wr_ref[0], preferred_element_type=F32)

    @pl.when(d == pl.num_programs(1) - 1)
    def _():
        k = ids[ME] % 2
        for o, kk in ((s_ref, k), (c_ref, 1 - k)):
            pair = acc.at[:, pl.ds(pl.multiple_of(kk * 512, 512), 512)]
            _emit_heads(pair, cos_ref, sin_ref, c == 2, [o.at[0, h] for h in range(2)])


def _qkv_own(ids, x0, x1, x2, x3, w_ref, tab_ref, ptab_ref, o_ref, xs, acc, wt, sem, buf, wsem):
    c, d = pl.program_id(0), pl.program_id(1)
    nd = pl.num_programs(1)
    bd, t = buf.shape[1], x0.shape[0]
    take = _stream(w_ref, buf, wsem, ids[OWN_HEAD])

    def copy(b, k):
        cols = pl.ds(pl.multiple_of(k * bd, bd), bd)
        return pltpu.make_async_copy((x0, x1, x2, x3)[b].at[:, cols], xs.at[pl.ds(b * t, t), cols], sem.at[k, b])

    @pl.when((c == 0) & (d == 0))
    def _():
        for k in range(x0.shape[1] // bd):
            for b in range(4):
                copy(b, k).start()

    @pl.when(d == 0)
    def _():
        acc[...] = jnp.zeros_like(acc)

    @pl.when(c == 0)
    def _():
        for b in range(4):
            copy(b, d).wait()

    wt[...] = take()
    cols = pl.ds(pl.multiple_of(d * bd, bd), bd)
    for h in range(2):
        for m in range(2):
            r = slice(m * 2 * t, (m + 1) * 2 * t)
            acc[r, h * 256:(h + 1) * 256] += jnp.dot(xs[r, cols], wt[:, h * 256:(h + 1) * 256],
                                                     preferred_element_type=F32)

    @pl.when(d == nd - 1)
    def _():
        for b in range(4):
            r = pl.ds(b * t, t)
            tb = (tab_ref, ptab_ref)[b % 2]
            tr = pl.ds((b // 2) * t, t)
            _emit_heads(acc.at[r], tb.at[0, tr], tb.at[1, tr], c == 2, [o_ref.at[b, 0, h] for h in range(2)])


def _qkv_next(ids, xn, w_ref, cos_ref, sin_ref, s_ref, c_ref, acc):
    c, j = pl.program_id(0), pl.program_id(1)

    acc[...] = jnp.dot(xn[...], w_ref[0], preferred_element_type=F32)
    for n, o_ref in enumerate((s_ref, c_ref)):
        @pl.when(j == n)
        def _():
            _emit_heads(acc, cos_ref, sin_ref, c == 2, [o_ref.at[0, h] for h in range(2)])


def _attend(masks, ids, l_ref, rs0, rs1, rc0, rc1, *refs):
    nq = len(masks)
    outs = refs[:2 * nq]
    qkv, m_s, l_s, acc, sem = refs[2 * nq:]
    src = [l_ref.at[b] for b in range(4)] + [rs0, rs1, rc0, rc1]
    t, dh = rs0.shape[2:]
    me = ids[ME]
    chips = [(me ^ m) // 2 for m in masks]
    last = functools.reduce(jnp.maximum, chips)

    def kv_copy(n, b):
        rows = pl.ds(pl.multiple_of(b * t, t), t)
        return pltpu.make_async_copy(src[n].at[pl.ds(1, 2)], qkv.at[pl.ds(1, 2), :, rows, :], sem.at[0, b])

    def q_copy(n, b):
        rows = pl.ds(pl.multiple_of(b * t, t), t)
        return pltpu.make_async_copy(src[n].at[0], qkv.at[0, :, rows, :], sem.at[1, b])

    def issue(want_chip, queries):
        for n in range(8):
            b = ids[SRC + n]

            @pl.when(b // 2 == want_chip)
            def _():
                if queries:
                    q_copy(n, b).start()
                else:
                    kv_copy(n, b).start()

    issue(chips[0], True)
    for j in range(4):
        @pl.when(j <= last)
        def _():
            issue(j, False)

        if j == 0:
            for cc in chips[1:]:
                issue(cc, True)

    k2 = (dh ** -0.5) * 1.4426950408889634

    k = me % 2

    def chip_rows(i, carry):
        cc = jnp.where(i == 0, chips[0], chips[1])
        q0 = pl.multiple_of(cc * 2 * t, 2 * t)
        for b in range(2):
            q_copy(0, 2 * cc + b).wait()
        m_s[...] = jnp.full_like(m_s, -jnp.inf)
        l_s[...] = jnp.zeros_like(l_s)
        acc[...] = jnp.zeros_like(acc)

        def kv_wait(j):
            @pl.when(i == 0)
            def _():
                for b in range(2):
                    kv_copy(0, 2 * j + b).wait()

        def tile(base, r0, nr, w, masked):
            rs = slice(r0, r0 + nr)
            ss = []
            for h in range(2):
                s = lax.dot_general(qkv[0, h, pl.ds(q0 + r0, nr), :], qkv[1, h, pl.ds(base, w), :],
                                    (((1,), (1,)), ((), ())), preferred_element_type=F32)
                if masked:
                    row = lax.broadcasted_iota(jnp.int32, (nr, w), 0)
                    col = lax.broadcasted_iota(jnp.int32, (nr, w), 1)
                    s = jnp.where(row >= col, s, -jnp.inf)
                ss.append(s)
            for h in range(2):
                ch = [ss[h][:, q * 128:(q + 1) * 128] for q in range(w // 128)]
                m_old = m_s[h, rs]
                m_new = jnp.maximum(m_old, jnp.max(functools.reduce(jnp.maximum, ch), axis=-1, keepdims=True))
                alpha = jnp.exp2((m_old - m_new) * k2)
                m_s[h, rs] = m_new
                mk = m_new * k2
                ps = [jnp.exp2(v * k2 - mk) for v in ch]
                l_s[h, rs] = l_s[h, rs] * alpha + functools.reduce(jnp.add, ps)
                p = jnp.concatenate([v.astype(BF) for v in ps], axis=1)
                pv = jnp.dot(p, qkv[2, h, pl.ds(base, w), :], preferred_element_type=F32)
                for q in range(dh // 128):
                    sl = slice(q * 128, (q + 1) * 128)
                    acc[h, rs, sl] = acc[h, rs, sl] * alpha + pv[:, sl]

        def body(j, carry):
            kv_wait(j)
            tile(pl.multiple_of(j * 2 * t, 2 * t), 0, 2 * t, 2 * t, False)
            return carry

        lax.fori_loop(0, cc, body, 0)
        kv_wait(cc)
        tile(q0, 0, t, t, True)
        tile(q0, t, t, t, False)
        tile(pl.multiple_of(q0 + t, t), t, t, t, True)

        @pl.when(i == 0)
        def _():
            def drain(j, carry):
                kv_wait(j)
                return carry

            lax.fori_loop(cc + 1, last + 1, drain, 0)

        for o in range(2):
            rs = pl.ds(pl.multiple_of((k if o == 0 else 1 - k) * t, t), t)
            for h in range(2):
                l = jnp.sum(l_s[h, rs, :], axis=-1, keepdims=True)
                v = (acc[h, rs, :] / l).astype(BF)
                for n in range(nq):
                    @pl.when(i == n)
                    def _(n=n):
                        outs[2 * n + o][:, h * dh:(h + 1) * dh] = v
        return carry

    lax.fori_loop(0, nq, chip_rows, 0)


def _project(n, ids, *refs):
    o = jnp.concatenate([r[...] for r in refs[:n]], axis=1)
    w = jnp.concatenate([r[...] for r in refs[n:2 * n]], axis=0)
    base, out = refs[2 * n], refs[2 * n + 1]
    tn = w.shape[1]
    cols = pl.ds(pl.multiple_of(pl.program_id(0) * tn, tn), tn)
    a = jnp.dot(o, w, preferred_element_type=F32)
    if out.shape[1] == tn:
        out[...] = (base[:, cols] + a).astype(BF)
    else:
        out[:, cols] = base[...].astype(F32) + a


def _params(limit=VMEM_LIMIT):
    return pltpu.CompilerParams(vmem_limit_bytes=limit)


def _cost(flops, nbytes):
    return pl.CostEstimate(flops=int(flops * COST), bytes_accessed=int(nbytes * COST), transcendentals=0)


def solution(mesh):
    rows = P(("data", "seq"), None)

    def local(x, g, wqkv, wo):
        t, d = x.shape
        _, _, hh, dh = wqkv.shape
        me = lax.axis_index("seq").astype(jnp.int32)
        k = me % 2
        kf, yf = 2 << k, 4 >> k

        def send(a, f):
            return lax.ppermute(a, "seq", [(i, f(i)) for i in range(8)])

        def to_a(i):
            return i ^ (2 << (i & 1))

        def to_same(i):
            return i ^ (4 >> (i & 1))

        def to_cross(i):
            return to_same(i) ^ 1

        inv = 10000.0 ** (-jnp.arange(dh // 2, dtype=F32) * 2.0 / dh)

        def tables(b):
            pos = (b[:, None] * t + jnp.arange(t)[None, :]).reshape(-1).astype(F32)
            ang = pos[:, None] * inv[None, :]
            return jnp.stack([jnp.cos(ang), jnp.sin(ang)])

        a_id, so, po = me ^ kf, me ^ yf, me ^ 1
        xo = po ^ kf

        ids = jnp.stack([me, so // 2 * 4, me * 2]
                        + [me, po, a_id, po ^ yf, so, me ^ 6, xo, me ^ 7]
                        + [me ^ m for m in range(8)]).astype(jnp.int32)
        tab = tables(jnp.stack([me, a_id]))
        g2 = g[None, :]

        xa = send(x, to_a)

        half = jax.ShapeDtypeStruct((3, 2, t, dh), BF)
        xn_shape = jax.ShapeDtypeStruct((t, d), BF)
        bd = 1024
        nd = d // bd
        flops = 2 * t * d * 12 * dh

        def partner(a):
            return send(a, lambda i: i ^ 1)

        def tiles(n):
            return [pltpu.VMEM((2, bd, n, dh), BF), pltpu.SemaphoreType.DMA((2,))]

        def tab_spec(n, b):
            return pl.BlockSpec((pl.Squeezed(), t, dh // 2), lambda *_: (n, b, 0))

        whole = pl.BlockSpec((t, d), lambda *_: (0, 0), pipeline_mode=pl.Buffered(1))
        anyspec = pl.BlockSpec(memory_space=pl.ANY)
        half2 = pl.BlockSpec((1, 2, t, dh), lambda c, *_: (c, 0, 0, 0))

        b_same, b_cross, w_b, xn_o = pl.pallas_call(
            _qkv_first,
            grid_spec=pltpu.PrefetchScalarGridSpec(
                num_scalar_prefetch=1, grid=(3, nd),
                in_specs=[whole, pl.BlockSpec((1, d), lambda *_: (0, 0)), anyspec,
                          tab_spec(0, 0), tab_spec(1, 0)],
                out_specs=[half2, half2, pl.BlockSpec((1, bd, 4 * dh), lambda c, i, s: (c, i, 0)), whole],
                scratch_shapes=[pltpu.VMEM((t, 4 * dh), F32)] + tiles(4)),
            out_shape=[half, half, jax.ShapeDtypeStruct((3, d, 4 * dh), BF), xn_shape],
            compiler_params=_params(), cost_estimate=_cost(flops * 2.5, 80e6), name="qkv_first",
        )(ids, x, g2, wqkv, tab, tab)
        rs_own, rc_own = send(b_same, to_same), send(b_cross, to_cross)
        xn_po, ptab = partner(xn_o), partner(tab)
        rb = 128
        xn_a = pl.pallas_call(
            _norm_rows, grid=(t // rb,),
            in_specs=[pl.BlockSpec((rb, d), lambda i: (i, 0)), pl.BlockSpec((1, d), lambda i: (0, 0))],
            out_specs=pl.BlockSpec((rb, d), lambda i: (i, 0)), out_shape=xn_shape,
            compiler_params=_params(), cost_estimate=_cost(2e9, 8e6), name="norm",
        )(xa, g2)
        xn_pa = partner(xn_a)
        a_same, a_cross = pl.pallas_call(
            _qkv_next,
            grid_spec=pltpu.PrefetchScalarGridSpec(
                num_scalar_prefetch=1, grid=(3, 2),
                in_specs=[whole, pl.BlockSpec((1, d, 2 * dh), lambda c, i, s: (c, 0, (i + s[ME]) % 2)),
                          tab_spec(0, 1), tab_spec(1, 1)],
                out_specs=[half2, half2],
                scratch_shapes=[pltpu.VMEM((t, 2 * dh), F32)]),
            out_shape=[half, half],
            compiler_params=_params(), cost_estimate=_cost(flops * 1.4, 35e6), name="qkv_next",
        )(ids, xn_a, w_b, tab, tab)
        rs_a, rc_a = send(a_same, to_same), send(a_cross, to_cross)
        both_tab = pl.BlockSpec((2, 2 * t, dh // 2), lambda *_: (0, 0, 0), pipeline_mode=pl.Buffered(1))
        loc = pl.pallas_call(
            _qkv_own,
            grid_spec=pltpu.PrefetchScalarGridSpec(
                num_scalar_prefetch=1, grid=(3, nd),
                in_specs=[anyspec] * 5 + [both_tab, both_tab],
                out_specs=pl.BlockSpec((4, 1, 2, t, dh), lambda c, i, s: (0, c, 0, 0, 0)),
                scratch_shapes=[pltpu.VMEM((4 * t, d), BF), pltpu.VMEM((4 * t, 2 * dh), F32),
                                pltpu.VMEM((bd, 2 * dh), BF), pltpu.SemaphoreType.DMA((nd, 4))]
                + tiles(2)),
            out_shape=jax.ShapeDtypeStruct((4, 3, 2, t, dh), BF),
            compiler_params=_params(), cost_estimate=_cost(flops * 2.8, 60e6), name="qkv_own",
        )(ids, xn_o, xn_po, xn_a, xn_pa, wqkv, tab, ptab)
        src = [loc, rs_own, rs_a, rc_own, rc_a]

        def attend(ms):
            nq = len(ms)
            return pl.pallas_call(
                functools.partial(_attend, ms),
                grid_spec=pltpu.PrefetchScalarGridSpec(
                    num_scalar_prefetch=1, grid=(1,),
                    in_specs=[anyspec] * 5,
                    out_specs=[pl.BlockSpec((t, 2 * dh), lambda i, s: (0, 0))] * (2 * nq),
                    scratch_shapes=[pltpu.VMEM((3, 2, 8 * t, dh), BF),
                                    pltpu.VMEM((2, 2 * t, 128), F32), pltpu.VMEM((2, 2 * t, 128), F32),
                                    pltpu.VMEM((2, 2 * t, dh), F32), pltpu.SemaphoreType.DMA((2, 8))]),
                out_shape=[jax.ShapeDtypeStruct((t, 2 * dh), BF)] * (2 * nq),
                compiler_params=_params(), cost_estimate=_cost(nq * 10e9, 13e6), name="attend",
            )(ids, *src)

        got = {}
        for ms in GROUPS:
            o = attend(ms)
            for i, m in enumerate(ms):
                for e in range(2):
                    v = m ^ e
                    got[v] = send(o[2 * i + e], lambda j, v=v: j ^ v) if v else o[2 * i + e]

        wo2 = wo.reshape(hh * dh, d)
        o_spec = pl.BlockSpec((t, 2 * dh), lambda i, s: (0, 0))

        def project(tn, ms, part=None):
            n = len(ms)

            def w_spec(m):
                return pl.BlockSpec((2 * dh, tn), lambda i, s: (s[DEV + m], i))

            col = pl.BlockSpec((t, tn), lambda i, s: (0, i))
            kept = pl.BlockSpec(memory_space=pltpu.VMEM)
            return pl.pallas_call(
                functools.partial(_project, n),
                grid_spec=pltpu.PrefetchScalarGridSpec(
                    num_scalar_prefetch=1, grid=(d // tn,),
                    in_specs=[o_spec] * n + [w_spec(m) for m in ms] + [col if part is None else kept],
                    out_specs=kept if part is None else col),
                out_shape=pltpu.VMEM((t, d), F32) if part is None else jax.ShapeDtypeStruct((t, d), BF),
                compiler_params=_params(PROJ_VMEM), cost_estimate=_cost(n * 2 * t * 2 * dh * d * 1.3, n * 4.2e6 + 8e6),
                name="project",
            )(ids, *[got[m] for m in ms], *[wo2] * n, x if part is None else part)

        part = project(TN0, (0, 1, 2, 3, 4, 5))
        return project(TN1, (6, 7), part)

    return jax.shard_map(local, mesh=mesh,
                         in_specs=(rows, P(None), P(None, None, None, None), P(None, None, None)),
                         out_specs=rows, check_vma=False)
```

```python
import functools

import jax
import jax.numpy as jnp
from jax import lax
from jax.experimental import pallas as pl
from jax.experimental.pallas import tpu as pltpu
from jax.sharding import PartitionSpec as P


BF = jnp.bfloat16
F32 = jnp.float32
VMEM_LIMIT = 62 << 20
PROJ_VMEM = 40 << 20
COST = 0.05
TN0, TN1 = 1024, 1024
GROUPS = ((2, 4), (6, 0))
ME, B_HEAD, OWN_HEAD, SRC, DEV = 0, 1, 2, 3, 11


def _norm(x_ref, g_ref, xn, base):
    rb = 16

    def body(i, c):
        r = pl.ds(pl.multiple_of(i * rb, rb), rb)
        xf = x_ref[r, :].astype(F32)
        ms = jnp.mean(xf * xf, axis=-1, keepdims=True)
        xn[pl.ds(pl.multiple_of(base + i * rb, rb), rb), :] = (xf * lax.rsqrt(ms + 1e-5) * g_ref[...]).astype(BF)
        return c

    lax.fori_loop(0, x_ref.shape[0] // rb, body, 0, unroll=2)


def _norm_rows(x_ref, g_ref, o_ref):
    _norm(x_ref, g_ref, o_ref, 0)


def _emit_heads(acc, cos, sin, is_v, outs):
    @pl.when(is_v)
    def _():
        for j, o in enumerate(outs):
            o[...] = acc[:, j * 256:(j + 1) * 256].astype(BF)

    @pl.when(jnp.logical_not(is_v))
    def _():
        cs, sn = cos[...], sin[...]
        for j, o in enumerate(outs):
            x1, x2 = acc[:, j * 256:j * 256 + 128], acc[:, j * 256 + 128:(j + 1) * 256]
            o[:, :128] = (x1 * cs - x2 * sn).astype(BF)
            o[:, 128:] = (x2 * cs + x1 * sn).astype(BF)


def _stream(w_ref, buf, sem, head):
    c, d = pl.program_id(0), pl.program_id(1)
    nc, nd = pl.num_programs(0), pl.num_programs(1)
    _, bd, n, dh = buf.shape
    i = c * nd + d

    def copy(j):
        rows = pl.ds(pl.multiple_of(lax.rem(j, nd) * bd, bd), bd)
        heads = pl.ds(pl.multiple_of(head, n), n)
        return pltpu.make_async_copy(w_ref.at[rows, j // nd, heads, :], buf.at[j % 2], sem.at[j % 2])

    @pl.when(i == 0)
    def _():
        copy(0).start()

    @pl.when(i + 1 < nc * nd)
    def _():
        copy(i + 1).start()

    def take():
        copy(i).wait()
        return buf[i % 2].reshape(bd, n * dh)

    return take


def _qkv_first(ids, x_ref, g_ref, w_ref, cos_ref, sin_ref, s_ref, c_ref, o_ref, wr_ref, xn, acc, acc2, wt,
               buf, wsem, buf2, wsem2):
    c, d = pl.program_id(0), pl.program_id(1)
    bd = buf.shape[1]
    take = _stream(w_ref, buf, wsem, ids[B_HEAD])
    take2 = _stream(w_ref, buf2, wsem2, ids[OWN_HEAD])

    @pl.when((c == 0) & (d == 0))
    def _():
        _norm(x_ref, g_ref, xn, 0)

    @pl.when(d == 0)
    def _():
        acc[...] = jnp.zeros_like(acc)
        acc2[...] = jnp.zeros_like(acc2)

    wr_ref[0] = take()
    xb = xn[:, pl.ds(pl.multiple_of(d * bd, bd), bd)]
    acc[...] += jnp.dot(xb, wr_ref[0], preferred_element_type=F32)
    wt[...] = take2()
    acc2[...] += jnp.dot(xb, wt[...], preferred_element_type=F32)

    @pl.when(d == pl.num_programs(1) - 1)
    def _():
        k = ids[ME] % 2
        for o, kk in ((s_ref, k), (c_ref, 1 - k)):
            pair = acc.at[:, pl.ds(pl.multiple_of(kk * 512, 512), 512)]
            _emit_heads(pair, cos_ref, sin_ref, c == 2, [o.at[0, h] for h in range(2)])
        _emit_heads(acc2, cos_ref, sin_ref, c == 2, [o_ref.at[0, h] for h in range(2)])


def _qkv_own(halves, ids, *refs):
    nb = len(halves)
    xr = refs[:nb]
    w_ref, tab_ref, ptab_ref, o_ref, xs, acc, wt, sem, buf, wsem = refs[nb:]
    c, d = pl.program_id(0), pl.program_id(1)
    nd = pl.num_programs(1)
    bd, t = buf.shape[1], xr[0].shape[0]
    take = _stream(w_ref, buf, wsem, ids[OWN_HEAD])

    def copy(b, k):
        cols = pl.ds(pl.multiple_of(k * bd, bd), bd)
        return pltpu.make_async_copy(xr[b].at[:, cols], xs.at[pl.ds(b * t, t), cols], sem.at[k, b])

    @pl.when((c == 0) & (d == 0))
    def _():
        for k in range(xr[0].shape[1] // bd):
            for b in range(nb):
                copy(b, k).start()

    @pl.when(d == 0)
    def _():
        acc[...] = jnp.zeros_like(acc)

    @pl.when(c == 0)
    def _():
        for b in range(nb):
            copy(b, d).wait()

    wt[...] = take()
    cols = pl.ds(pl.multiple_of(d * bd, bd), bd)
    acc[...] += jnp.dot(xs[:, cols], wt[...], preferred_element_type=F32)

    @pl.when(d == nd - 1)
    def _():
        for b, (n, half) in enumerate(halves):
            tb = (tab_ref, ptab_ref)[n]
            r, tr = pl.ds(b * t, t), pl.ds(half * t, t)
            _emit_heads(acc.at[r], tb.at[0, tr], tb.at[1, tr], c == 2, [o_ref.at[b, 0, h] for h in range(2)])


def _qkv_next(ids, xn, w_ref, cos_ref, sin_ref, qs_ref, qc_ref, s_ref, c_ref, acc):
    c, j = pl.program_id(0), pl.program_id(1)
    acc[...] = jnp.dot(xn[...], w_ref[0], preferred_element_type=F32)
    for n, (q_ref, o_ref) in enumerate(((qs_ref, s_ref), (qc_ref, c_ref))):
        @pl.when((j == n) & (c == 0))
        def _():
            _emit_heads(acc, cos_ref, sin_ref, c == 2, [q_ref.at[0, h] for h in range(2)])

        @pl.when((j == n) & (c > 0))
        def _():
            _emit_heads(acc, cos_ref, sin_ref, c == 2, [o_ref.at[0, h] for h in range(2)])


def _attend(masks, ids, lo, lr, rs0, rs1, rc0, rc1, qs1, qc1, *refs):
    nq = len(masks)
    outs = refs[:2 * nq]
    qkv, m_s, l_s, acc, sem = refs[2 * nq:]
    kv = pl.ds(1, 2)
    q_src = [lo.at[0]] + [lr.at[b, 0] for b in range(3)] + [rs0.at[0], qs1.at[0], rc0.at[0], qc1.at[0]]
    kv_src = [lo.at[kv]] + [lr.at[b, kv] for b in range(3)] + [rs0.at[kv], rs1, rc0.at[kv], rc1]
    t, dh = rs0.shape[2:]
    me = ids[ME]
    chips = [(me ^ m) // 2 for m in masks]
    last = functools.reduce(jnp.maximum, chips)

    def kv_copy(n, b):
        rows = pl.ds(pl.multiple_of(b * t, t), t)
        return pltpu.make_async_copy(kv_src[n], qkv.at[kv, :, rows, :], sem.at[0, b])

    def q_copy(n, b):
        rows = pl.ds(pl.multiple_of(b * t, t), t)
        return pltpu.make_async_copy(q_src[n], qkv.at[0, :, rows, :], sem.at[1, b])

    def issue(want_chip, queries):
        for n in range(8):
            b = ids[SRC + n]

            @pl.when(b // 2 == want_chip)
            def _():
                if queries:
                    q_copy(n, b).start()
                else:
                    kv_copy(n, b).start()

    issue(chips[0], True)
    for j in range(4):
        @pl.when(j <= last)
        def _():
            issue(j, False)

        if j == 0:
            for cc in chips[1:]:
                issue(cc, True)

    k2 = (dh ** -0.5) * 1.4426950408889634

    k = me % 2

    def chip_rows(i, carry):
        cc = jnp.where(i == 0, chips[0], chips[1])
        q0 = pl.multiple_of(cc * 2 * t, 2 * t)
        for b in range(2):
            q_copy(0, 2 * cc + b).wait()
        m_s[...] = jnp.full_like(m_s, -jnp.inf)
        l_s[...] = jnp.zeros_like(l_s)
        acc[...] = jnp.zeros_like(acc)

        def kv_wait(j):
            @pl.when(i == 0)
            def _():
                for b in range(2):
                    kv_copy(0, 2 * j + b).wait()

        def tile(base, r0, nr, w, masked):
            rs = slice(r0, r0 + nr)
            ss = []
            for h in range(2):
                s = lax.dot_general(qkv[0, h, pl.ds(q0 + r0, nr), :], qkv[1, h, pl.ds(base, w), :],
                                    (((1,), (1,)), ((), ())), preferred_element_type=F32)
                if masked:
                    row = lax.broadcasted_iota(jnp.int32, (nr, w), 0)
                    col = lax.broadcasted_iota(jnp.int32, (nr, w), 1)
                    s = jnp.where(row >= col, s, -jnp.inf)
                ss.append(s)
            for h in range(2):
                ch = [ss[h][:, q * 128:(q + 1) * 128] for q in range(w // 128)]
                m_old = m_s[h, rs]
                m_new = jnp.maximum(m_old, jnp.max(functools.reduce(jnp.maximum, ch), axis=-1, keepdims=True))
                alpha = jnp.exp2((m_old - m_new) * k2)
                m_s[h, rs] = m_new
                mk = m_new * k2
                ps = [jnp.exp2(v * k2 - mk) for v in ch]
                l_s[h, rs] = l_s[h, rs] * alpha + functools.reduce(jnp.add, ps)
                p = jnp.concatenate([v.astype(BF) for v in ps], axis=1)
                pv = jnp.dot(p, qkv[2, h, pl.ds(base, w), :], preferred_element_type=F32)
                for q in range(dh // 128):
                    sl = slice(q * 128, (q + 1) * 128)
                    acc[h, rs, sl] = acc[h, rs, sl] * alpha + pv[:, sl]

        def body(j, carry):
            kv_wait(j)
            tile(pl.multiple_of(j * 2 * t, 2 * t), 0, 2 * t, 2 * t, False)
            return carry

        lax.fori_loop(0, cc, body, 0)
        kv_wait(cc)
        tile(q0, 0, t, t, True)
        tile(q0, t, t, t, False)
        tile(pl.multiple_of(q0 + t, t), t, t, t, True)

        @pl.when(i == 0)
        def _():
            def drain(j, carry):
                kv_wait(j)
                return carry

            lax.fori_loop(cc + 1, last + 1, drain, 0)

        for o in range(2):
            rs = pl.ds(pl.multiple_of((k if o == 0 else 1 - k) * t, t), t)
            for h in range(2):
                l = jnp.sum(l_s[h, rs, :], axis=-1, keepdims=True)
                v = (acc[h, rs, :] / l).astype(BF)
                for n in range(nq):
                    @pl.when(i == n)
                    def _(n=n):
                        outs[2 * n + o][:, h * dh:(h + 1) * dh] = v
        return carry

    lax.fori_loop(0, nq, chip_rows, 0)


def _project(n, ids, *refs):
    o = jnp.concatenate([r[...] for r in refs[:n]], axis=1)
    w = jnp.concatenate([r[...] for r in refs[n:2 * n]], axis=0)
    base, out = refs[2 * n], refs[2 * n + 1]
    tn = w.shape[1]
    cols = pl.ds(pl.multiple_of(pl.program_id(0) * tn, tn), tn)
    a = jnp.dot(o, w, preferred_element_type=F32)
    if out.shape[1] == tn:
        out[...] = (base[:, cols] + a).astype(BF)
    else:
        out[:, cols] = base[...].astype(F32) + a


def _params(limit=VMEM_LIMIT):
    return pltpu.CompilerParams(vmem_limit_bytes=limit)


def _cost(flops, nbytes):
    return pl.CostEstimate(flops=int(flops * COST), bytes_accessed=int(nbytes * COST), transcendentals=0)


def solution(mesh):
    rows = P(("data", "seq"), None)

    def local(x, g, wqkv, wo):
        t, d = x.shape
        _, _, hh, dh = wqkv.shape
        me = lax.axis_index("seq").astype(jnp.int32)
        k = me % 2
        kf, yf = 2 << k, 4 >> k

        def send(a, f):
            return lax.ppermute(a, "seq", [(i, f(i)) for i in range(8)])

        def to_a(i):
            return i ^ (2 << (i & 1))

        def to_same(i):
            return i ^ (4 >> (i & 1))

        def to_cross(i):
            return to_same(i) ^ 1

        inv = 10000.0 ** (-jnp.arange(dh // 2, dtype=F32) * 2.0 / dh)

        def tables(b):
            pos = (b[:, None] * t + jnp.arange(t)[None, :]).reshape(-1).astype(F32)
            ang = pos[:, None] * inv[None, :]
            return jnp.stack([jnp.cos(ang), jnp.sin(ang)])

        a_id, so, po = me ^ kf, me ^ yf, me ^ 1
        xo = po ^ kf

        ids = jnp.stack([me, so // 2 * 4, me * 2]
                        + [me, po, a_id, po ^ yf, so, me ^ 6, xo, me ^ 7]
                        + [me ^ m for m in range(8)]).astype(jnp.int32)
        tab = tables(jnp.stack([me, a_id]))
        g2 = g[None, :]

        xa = send(x, to_a)

        half = jax.ShapeDtypeStruct((3, 2, t, dh), BF)
        xn_shape = jax.ShapeDtypeStruct((t, d), BF)
        bd = 1024
        nd = d // bd
        flops = 2 * t * d * 12 * dh

        def partner(a):
            return send(a, lambda i: i ^ 1)

        def tiles(n):
            return [pltpu.VMEM((2, bd, n, dh), BF), pltpu.SemaphoreType.DMA((2,))]

        def tab_spec(n, b):
            return pl.BlockSpec((pl.Squeezed(), t, dh // 2), lambda *_: (n, b, 0))

        whole = pl.BlockSpec((t, d), lambda *_: (0, 0), pipeline_mode=pl.Buffered(1))
        anyspec = pl.BlockSpec(memory_space=pl.ANY)
        half2 = pl.BlockSpec((1, 2, t, dh), lambda c, *_: (c, 0, 0, 0))

        b_same, b_cross, loc_o, w_b, xn_o = pl.pallas_call(
            _qkv_first,
            grid_spec=pltpu.PrefetchScalarGridSpec(
                num_scalar_prefetch=1, grid=(3, nd),
                in_specs=[whole, pl.BlockSpec((1, d), lambda *_: (0, 0)), anyspec,
                          tab_spec(0, 0), tab_spec(1, 0)],
                out_specs=[half2, half2, half2, pl.BlockSpec((1, bd, 4 * dh), lambda c, i, s: (c, i, 0)), whole],
                scratch_shapes=[pltpu.VMEM((t, 4 * dh), F32), pltpu.VMEM((t, 2 * dh), F32),
                                pltpu.VMEM((bd, 2 * dh), BF)] + tiles(4) + tiles(2)),
            out_shape=[half, half, half, jax.ShapeDtypeStruct((3, d, 4 * dh), BF), xn_shape],
            compiler_params=_params(), cost_estimate=_cost(flops * 2.5, 80e6), name="qkv_first",
        )(ids, x, g2, wqkv, tab, tab)
        both_tab = pl.BlockSpec((2, 2 * t, dh // 2), lambda *_: (0, 0, 0), pipeline_mode=pl.Buffered(1))

        def own(xs, halves, ptab):
            n = len(xs)
            return pl.pallas_call(
                functools.partial(_qkv_own, halves),
                grid_spec=pltpu.PrefetchScalarGridSpec(
                    num_scalar_prefetch=1, grid=(3, nd),
                    in_specs=[anyspec] * (n + 1) + [both_tab, both_tab],
                    out_specs=pl.BlockSpec((n, 1, 2, t, dh), lambda c, i, s: (0, c, 0, 0, 0)),
                    scratch_shapes=[pltpu.VMEM((n * t, d), BF), pltpu.VMEM((n * t, 2 * dh), F32),
                                    pltpu.VMEM((bd, 2 * dh), BF), pltpu.SemaphoreType.DMA((nd, n))]
                    + tiles(2)),
                out_shape=jax.ShapeDtypeStruct((n, 3, 2, t, dh), BF),
                compiler_params=_params(), cost_estimate=_cost(flops * 0.7 * n, 15e6 + n * 6e6), name="qkv_own",
            )(ids, *xs, wqkv, tab, ptab)

        rs_own, rc_own = send(b_same, to_same), send(b_cross, to_cross)
        xn_po, ptab = partner(xn_o), partner(tab)
        rb = 128
        xn_a = pl.pallas_call(
            _norm_rows, grid=(t // rb,),
            in_specs=[pl.BlockSpec((rb, d), lambda i: (i, 0)), pl.BlockSpec((1, d), lambda i: (0, 0))],
            out_specs=pl.BlockSpec((rb, d), lambda i: (i, 0)), out_shape=xn_shape,
            compiler_params=_params(), cost_estimate=_cost(2e9, 8e6), name="norm",
        )(xa, g2)
        xn_pa = partner(xn_a)
        q_same, q_cross, a_same, a_cross = pl.pallas_call(
            _qkv_next,
            grid_spec=pltpu.PrefetchScalarGridSpec(
                num_scalar_prefetch=1, grid=(3, 2),
                in_specs=[whole, pl.BlockSpec((1, d, 2 * dh), lambda c, i, s: (c, 0, (i + s[ME]) % 2)),
                          tab_spec(0, 1), tab_spec(1, 1)],
                out_specs=[pl.BlockSpec((1, 2, t, dh), lambda *_: (0, 0, 0, 0))] * 2
                + [pl.BlockSpec((1, 2, t, dh), lambda c, *_: (jnp.maximum(c - 1, 0), 0, 0, 0))] * 2,
                scratch_shapes=[pltpu.VMEM((t, 2 * dh), F32)]),
            out_shape=[jax.ShapeDtypeStruct((n, 2, t, dh), BF) for n in (1, 1, 2, 2)],
            compiler_params=_params(), cost_estimate=_cost(flops * 1.4, 35e6), name="qkv_next",
        )(ids, xn_a, w_b, tab, tab)
        rs_a, rc_a = send(a_same, to_same), send(a_cross, to_cross)
        rs_q, rc_q = send(q_same, to_same), send(q_cross, to_cross)
        loc_r = own((xn_po, xn_a, xn_pa), ((1, 0), (0, 1), (1, 1)), ptab)

        def attend(ms):
            nq = len(ms)
            return pl.pallas_call(
                functools.partial(_attend, ms),
                grid_spec=pltpu.PrefetchScalarGridSpec(
                    num_scalar_prefetch=1, grid=(1,),
                    in_specs=[anyspec] * 8,
                    out_specs=[pl.BlockSpec((t, 2 * dh), lambda i, s: (0, 0))] * (2 * nq),
                    scratch_shapes=[pltpu.VMEM((3, 2, 8 * t, dh), BF),
                                    pltpu.VMEM((2, 2 * t, 128), F32), pltpu.VMEM((2, 2 * t, 128), F32),
                                    pltpu.VMEM((2, 2 * t, dh), F32), pltpu.SemaphoreType.DMA((2, 8))]),
                out_shape=[jax.ShapeDtypeStruct((t, 2 * dh), BF)] * (2 * nq),
                compiler_params=_params(), cost_estimate=_cost(nq * 10e9, 13e6), name="attend",
            )(ids, loc_o, loc_r, rs_own, rs_a, rc_own, rc_a, *((rs_q, rc_q) if 6 in ms else (rs_a, rc_a)))

        got = {}
        for ms in GROUPS:
            o = attend(ms)
            for i, m in enumerate(ms):
                for e in range(2):
                    v = m ^ e
                    got[v] = send(o[2 * i + e], lambda j, v=v: j ^ v) if v else o[2 * i + e]

        wo2 = wo.reshape(hh * dh, d)
        o_spec = pl.BlockSpec((t, 2 * dh), lambda i, s: (0, 0))

        def project(tn, ms, part=None):
            n = len(ms)

            def w_spec(m):
                return pl.BlockSpec((2 * dh, tn), lambda i, s: (s[DEV + m], i))

            col = pl.BlockSpec((t, tn), lambda i, s: (0, i))
            kept = pl.BlockSpec(memory_space=pltpu.VMEM)
            return pl.pallas_call(
                functools.partial(_project, n),
                grid_spec=pltpu.PrefetchScalarGridSpec(
                    num_scalar_prefetch=1, grid=(d // tn,),
                    in_specs=[o_spec] * n + [w_spec(m) for m in ms] + [col if part is None else kept],
                    out_specs=kept if part is None else col),
                out_shape=pltpu.VMEM((t, d), F32) if part is None else jax.ShapeDtypeStruct((t, d), BF),
                compiler_params=_params(PROJ_VMEM), cost_estimate=_cost(n * 2 * t * 2 * dh * d * 1.3, n * 4.2e6 + 8e6),
                name="project",
            )(ids, *[got[m] for m in ms], *[wo2] * n, x if part is None else part)

        part = project(TN0, (0, 1, 2, 3, 4, 5))
        return project(TN1, (6, 7), part)

    return jax.shard_map(local, mesh=mesh,
                         in_specs=(rows, P(None), P(None, None, None, None), P(None, None, None)),
                         out_specs=rows, check_vma=False)
```

```python
import functools

import jax
import jax.numpy as jnp
from jax import lax
from jax.experimental import pallas as pl
from jax.experimental.pallas import tpu as pltpu
from jax.sharding import PartitionSpec as P


BF = jnp.bfloat16
F32 = jnp.float32
VMEM_LIMIT = 62 << 20
PROJ_VMEM = 40 << 20
COST = 0.05
TN0, TN1 = 1024, 1024
GROUPS = ((2, 4), (6, 0))
ME, B_HEAD, OWN_HEAD, SRC, DEV = 0, 1, 2, 3, 11


def _norm(x_ref, g_ref, xn):
    rb, d = 16, x_ref.shape[1]
    cols = [slice(j * 128, (j + 1) * 128) for j in range(d // 128)]

    def body(i, carry):
        r = pl.ds(pl.multiple_of(i * rb, rb), rb)
        parts = [jnp.zeros((rb, 128), F32)] * 4
        for j, c in enumerate(cols):
            v = x_ref[r, c].astype(F32)
            parts[j % 4] = parts[j % 4] + v * v
        ss = jnp.sum((parts[0] + parts[1]) + (parts[2] + parts[3]), axis=-1, keepdims=True)
        inv = jnp.broadcast_to(lax.rsqrt(ss * (1.0 / d) + 1e-5), (rb, 128))
        for c in cols:
            xn[r, c] = (x_ref[r, c].astype(F32) * inv * g_ref[:, c]).astype(BF)
        return carry

    lax.fori_loop(0, x_ref.shape[0] // rb, body, 0, unroll=8)


def _norm_rows(x_ref, g_ref, o_ref):
    _norm(x_ref, g_ref, o_ref)


def _emit_heads(acc, cos, sin, is_v, outs):
    @pl.when(is_v)
    def _():
        for j, o in enumerate(outs):
            o[...] = acc[:, j * 256:(j + 1) * 256].astype(BF)

    @pl.when(jnp.logical_not(is_v))
    def _():
        cs, sn = cos[...], sin[...]
        for j, o in enumerate(outs):
            x1, x2 = acc[:, j * 256:j * 256 + 128], acc[:, j * 256 + 128:(j + 1) * 256]
            o[:, :128] = (x1 * cs - x2 * sn).astype(BF)
            o[:, 128:] = (x2 * cs + x1 * sn).astype(BF)


def _stream(w_ref, buf, sem, head):
    c, d = pl.program_id(0), pl.program_id(1)
    nc, nd = pl.num_programs(0), pl.num_programs(1)
    _, bd, n, dh = buf.shape
    i = c * nd + d

    def copy(j):
        rows = pl.ds(pl.multiple_of(lax.rem(j, nd) * bd, bd), bd)
        heads = pl.ds(pl.multiple_of(head, n), n)
        return pltpu.make_async_copy(w_ref.at[rows, j // nd, heads, :], buf.at[j % 2], sem.at[j % 2])

    @pl.when(i == 0)
    def _():
        copy(0).start()

    @pl.when(i + 1 < nc * nd)
    def _():
        copy(i + 1).start()

    def take():
        copy(i).wait()
        return buf[i % 2].reshape(bd, n * dh)

    return take


def _qkv_first(ids, x_ref, g_ref, w_ref, cos_ref, sin_ref, s_ref, c_ref, o_ref, wr_ref, xn, acc, acc2, wt,
               buf, wsem, buf2, wsem2):
    c, d = pl.program_id(0), pl.program_id(1)
    bd = buf.shape[1]
    take = _stream(w_ref, buf, wsem, ids[B_HEAD])
    take2 = _stream(w_ref, buf2, wsem2, ids[OWN_HEAD])

    @pl.when((c == 0) & (d == 0))
    def _():
        _norm(x_ref, g_ref, xn)

    @pl.when(d == 0)
    def _():
        acc[...] = jnp.zeros_like(acc)
        acc2[...] = jnp.zeros_like(acc2)

    wr_ref[0] = take()
    xb = xn[:, pl.ds(pl.multiple_of(d * bd, bd), bd)]
    acc[...] += jnp.dot(xb, wr_ref[0], preferred_element_type=F32)
    wt[...] = take2()
    acc2[...] += jnp.dot(xb, wt[...], preferred_element_type=F32)

    @pl.when(d == pl.num_programs(1) - 1)
    def _():
        k = ids[ME] % 2
        for o, kk in ((s_ref, k), (c_ref, 1 - k)):
            pair = acc.at[:, pl.ds(pl.multiple_of(kk * 512, 512), 512)]
            _emit_heads(pair, cos_ref, sin_ref, c == 2, [o.at[0, h] for h in range(2)])
        _emit_heads(acc2, cos_ref, sin_ref, c == 2, [o_ref.at[0, h] for h in range(2)])


def _qkv_own(halves, ids, *refs):
    nb = len(halves)
    xr = refs[:nb]
    w_ref, tab_ref, ptab_ref, o_ref, xs, acc, wt, sem, buf, wsem = refs[nb:]
    c, d = pl.program_id(0), pl.program_id(1)
    nd = pl.num_programs(1)
    bd, t = buf.shape[1], xr[0].shape[0]
    take = _stream(w_ref, buf, wsem, ids[OWN_HEAD])

    def copy(b, k):
        cols = pl.ds(pl.multiple_of(k * bd, bd), bd)
        return pltpu.make_async_copy(xr[b].at[:, cols], xs.at[pl.ds(b * t, t), cols], sem.at[k, b])

    @pl.when((c == 0) & (d == 0))
    def _():
        for k in range(xr[0].shape[1] // bd):
            for b in range(nb):
                copy(b, k).start()

    @pl.when(d == 0)
    def _():
        acc[...] = jnp.zeros_like(acc)

    @pl.when(c == 0)
    def _():
        for b in range(nb):
            copy(b, d).wait()

    wt[...] = take()
    cols = pl.ds(pl.multiple_of(d * bd, bd), bd)
    acc[...] += jnp.dot(xs[:, cols], wt[...], preferred_element_type=F32)

    @pl.when(d == nd - 1)
    def _():
        for b, (n, half) in enumerate(halves):
            tb = (tab_ref, ptab_ref)[n]
            r, tr = pl.ds(b * t, t), pl.ds(half * t, t)
            _emit_heads(acc.at[r], tb.at[0, tr], tb.at[1, tr], c == 2, [o_ref.at[b, 0, h] for h in range(2)])


def _qkv_next(ids, xn, w_ref, cos_ref, sin_ref, qs_ref, qc_ref, s_ref, c_ref, acc):
    c, j = pl.program_id(0), pl.program_id(1)
    acc[...] = jnp.dot(xn[...], w_ref[0], preferred_element_type=F32)
    for n, (q_ref, o_ref) in enumerate(((qs_ref, s_ref), (qc_ref, c_ref))):
        @pl.when((j == n) & (c == 0))
        def _():
            _emit_heads(acc, cos_ref, sin_ref, c == 2, [q_ref.at[0, h] for h in range(2)])

        @pl.when((j == n) & (c > 0))
        def _():
            _emit_heads(acc, cos_ref, sin_ref, c == 2, [o_ref.at[0, h] for h in range(2)])


def _attend(masks, ids, lo, lr, rs0, rs1, rc0, rc1, qs1, qc1, *refs):
    nq = len(masks)
    outs = refs[:2 * nq]
    qkv, m_s, l_s, acc, sem = refs[2 * nq:]
    kv = pl.ds(1, 2)
    q_src = [lo.at[0]] + [lr.at[b, 0] for b in range(3)] + [rs0.at[0], qs1.at[0], rc0.at[0], qc1.at[0]]
    kv_src = [lo.at[kv]] + [lr.at[b, kv] for b in range(3)] + [rs0.at[kv], rs1, rc0.at[kv], rc1]
    t, dh = rs0.shape[2:]
    me = ids[ME]
    chips = [(me ^ m) // 2 for m in masks]
    last = functools.reduce(jnp.maximum, chips)

    def kv_copy(n, b):
        rows = pl.ds(pl.multiple_of(b * t, t), t)
        return pltpu.make_async_copy(kv_src[n], qkv.at[kv, :, rows, :], sem.at[0, b])

    def q_copy(n, b):
        rows = pl.ds(pl.multiple_of(b * t, t), t)
        return pltpu.make_async_copy(q_src[n], qkv.at[0, :, rows, :], sem.at[1, b])

    def issue(want_chip, queries):
        for n in range(8):
            b = ids[SRC + n]

            @pl.when(b // 2 == want_chip)
            def _():
                if queries:
                    q_copy(n, b).start()
                else:
                    kv_copy(n, b).start()

    issue(chips[0], True)
    for j in range(4):
        @pl.when(j <= last)
        def _():
            issue(j, False)

        if j == 0:
            for cc in chips[1:]:
                issue(cc, True)

    k2 = (dh ** -0.5) * 1.4426950408889634

    k = me % 2

    def chip_rows(i, carry):
        cc = jnp.where(i == 0, chips[0], chips[1])
        q0 = pl.multiple_of(cc * 2 * t, 2 * t)
        for b in range(2):
            q_copy(0, 2 * cc + b).wait()
        m_s[...] = jnp.full_like(m_s, -jnp.inf)
        l_s[...] = jnp.zeros_like(l_s)
        acc[...] = jnp.zeros_like(acc)

        def kv_wait(j):
            @pl.when(i == 0)
            def _():
                for b in range(2):
                    kv_copy(0, 2 * j + b).wait()

        def tile(base, r0, nr, w, masked):
            rs = slice(r0, r0 + nr)
            ss = []
            for h in range(2):
                s = lax.dot_general(qkv[0, h, pl.ds(q0 + r0, nr), :], qkv[1, h, pl.ds(base, w), :],
                                    (((1,), (1,)), ((), ())), preferred_element_type=F32)
                if masked:
                    row = lax.broadcasted_iota(jnp.int32, (nr, w), 0)
                    col = lax.broadcasted_iota(jnp.int32, (nr, w), 1)
                    s = jnp.where(row >= col, s, -jnp.inf)
                ss.append(s)
            for h in range(2):
                ch = [ss[h][:, q * 128:(q + 1) * 128] for q in range(w // 128)]
                m_old = m_s[h, rs]
                m_new = jnp.maximum(m_old, jnp.max(functools.reduce(jnp.maximum, ch), axis=-1, keepdims=True))
                alpha = jnp.exp2((m_old - m_new) * k2)
                m_s[h, rs] = m_new
                mk = m_new * k2
                ps = [jnp.exp2(v * k2 - mk) for v in ch]
                l_s[h, rs] = l_s[h, rs] * alpha + functools.reduce(jnp.add, ps)
                p = jnp.concatenate([v.astype(BF) for v in ps], axis=1)
                pv = jnp.dot(p, qkv[2, h, pl.ds(base, w), :], preferred_element_type=F32)
                for q in range(dh // 128):
                    sl = slice(q * 128, (q + 1) * 128)
                    acc[h, rs, sl] = acc[h, rs, sl] * alpha + pv[:, sl]

        def body(j, carry):
            kv_wait(j)
            tile(pl.multiple_of(j * 2 * t, 2 * t), 0, 2 * t, 2 * t, False)
            return carry

        lax.fori_loop(0, cc, body, 0)
        kv_wait(cc)
        tile(q0, 0, t, t, True)
        tile(q0, t, t, t, False)
        tile(pl.multiple_of(q0 + t, t), t, t, t, True)

        @pl.when(i == 0)
        def _():
            def drain(j, carry):
                kv_wait(j)
                return carry

            lax.fori_loop(cc + 1, last + 1, drain, 0)

        for o in range(2):
            rs = pl.ds(pl.multiple_of((k if o == 0 else 1 - k) * t, t), t)
            for h in range(2):
                l = jnp.sum(l_s[h, rs, :], axis=-1, keepdims=True)
                v = (acc[h, rs, :] / l).astype(BF)
                for n in range(nq):
                    @pl.when(i == n)
                    def _(n=n):
                        outs[2 * n + o][:, h * dh:(h + 1) * dh] = v
        return carry

    lax.fori_loop(0, nq, chip_rows, 0)


def _project(n, ids, *refs):
    o = jnp.concatenate([r[...] for r in refs[:n]], axis=1)
    w = jnp.concatenate([r[...] for r in refs[n:2 * n]], axis=0)
    base, out = refs[2 * n], refs[2 * n + 1]
    tn = w.shape[1]
    cols = pl.ds(pl.multiple_of(pl.program_id(0) * tn, tn), tn)
    a = jnp.dot(o, w, preferred_element_type=F32)
    if out.shape[1] == tn:
        out[...] = (base[:, cols] + a).astype(BF)
    else:
        out[:, cols] = base[...].astype(F32) + a


def _params(limit=VMEM_LIMIT):
    return pltpu.CompilerParams(vmem_limit_bytes=limit)


def _cost(flops, nbytes):
    return pl.CostEstimate(flops=int(flops * COST), bytes_accessed=int(nbytes * COST), transcendentals=0)


def solution(mesh):
    rows = P(("data", "seq"), None)

    def local(x, g, wqkv, wo):
        t, d = x.shape
        _, _, hh, dh = wqkv.shape
        me = lax.axis_index("seq").astype(jnp.int32)
        k = me % 2
        kf, yf = 2 << k, 4 >> k

        def send(a, f):
            return lax.ppermute(a, "seq", [(i, f(i)) for i in range(8)])

        def to_a(i):
            return i ^ (2 << (i & 1))

        def to_same(i):
            return i ^ (4 >> (i & 1))

        def to_cross(i):
            return to_same(i) ^ 1

        inv = 10000.0 ** (-jnp.arange(dh // 2, dtype=F32) * 2.0 / dh)

        def tables(b):
            pos = (b[:, None] * t + jnp.arange(t)[None, :]).reshape(-1).astype(F32)
            ang = pos[:, None] * inv[None, :]
            return jnp.stack([jnp.cos(ang), jnp.sin(ang)])

        a_id, so, po = me ^ kf, me ^ yf, me ^ 1
        xo = po ^ kf

        ids = jnp.stack([me, so // 2 * 4, me * 2]
                        + [me, po, a_id, po ^ yf, so, me ^ 6, xo, me ^ 7]
                        + [me ^ m for m in range(8)]).astype(jnp.int32)
        tab = tables(jnp.stack([me, a_id]))
        g2 = g[None, :]

        xa = send(x, to_a)

        half = jax.ShapeDtypeStruct((3, 2, t, dh), BF)
        xn_shape = jax.ShapeDtypeStruct((t, d), BF)
        bd = 1024
        nd = d // bd
        flops = 2 * t * d * 12 * dh

        def partner(a):
            return send(a, lambda i: i ^ 1)

        def tiles(n):
            return [pltpu.VMEM((2, bd, n, dh), BF), pltpu.SemaphoreType.DMA((2,))]

        def tab_spec(n, b):
            return pl.BlockSpec((pl.Squeezed(), t, dh // 2), lambda *_: (n, b, 0))

        whole = pl.BlockSpec((t, d), lambda *_: (0, 0), pipeline_mode=pl.Buffered(1))
        anyspec = pl.BlockSpec(memory_space=pl.ANY)
        half2 = pl.BlockSpec((1, 2, t, dh), lambda c, *_: (c, 0, 0, 0))

        b_same, b_cross, loc_o, w_b, xn_o = pl.pallas_call(
            _qkv_first,
            grid_spec=pltpu.PrefetchScalarGridSpec(
                num_scalar_prefetch=1, grid=(3, nd),
                in_specs=[whole, pl.BlockSpec((1, d), lambda *_: (0, 0)), anyspec,
                          tab_spec(0, 0), tab_spec(1, 0)],
                out_specs=[half2, half2, half2, pl.BlockSpec((1, bd, 4 * dh), lambda c, i, s: (c, i, 0)), whole],
                scratch_shapes=[pltpu.VMEM((t, 4 * dh), F32), pltpu.VMEM((t, 2 * dh), F32),
                                pltpu.VMEM((bd, 2 * dh), BF)] + tiles(4) + tiles(2)),
            out_shape=[half, half, half, jax.ShapeDtypeStruct((3, d, 4 * dh), BF), xn_shape],
            compiler_params=_params(), cost_estimate=_cost(flops * 2.5, 80e6), name="qkv_first",
        )(ids, x, g2, wqkv, tab, tab)
        both_tab = pl.BlockSpec((2, 2 * t, dh // 2), lambda *_: (0, 0, 0), pipeline_mode=pl.Buffered(1))

        def own(xs, halves, ptab):
            n = len(xs)
            return pl.pallas_call(
                functools.partial(_qkv_own, halves),
                grid_spec=pltpu.PrefetchScalarGridSpec(
                    num_scalar_prefetch=1, grid=(3, 2),
                    in_specs=[anyspec] * (n + 1) + [both_tab, both_tab],
                    out_specs=pl.BlockSpec((n, 1, 2, t, dh), lambda c, i, s: (0, c, 0, 0, 0)),
                    scratch_shapes=[pltpu.VMEM((n * t, d), BF), pltpu.VMEM((n * t, 2 * dh), F32),
                                    pltpu.VMEM((2048, 2 * dh), BF), pltpu.SemaphoreType.DMA((2, n))]
                    + [pltpu.VMEM((2, 2048, 2, dh), BF), pltpu.SemaphoreType.DMA((2,))]),
                out_shape=jax.ShapeDtypeStruct((n, 3, 2, t, dh), BF),
                compiler_params=_params(), cost_estimate=_cost(flops * 0.7 * n, 15e6 + n * 6e6), name="qkv_own",
            )(ids, *xs, wqkv, tab, ptab)

        rs_own, rc_own = send(b_same, to_same), send(b_cross, to_cross)
        xn_po, ptab = partner(xn_o), partner(tab)
        rb = 256
        xn_a = pl.pallas_call(
            _norm_rows, grid=(t // rb,),
            in_specs=[pl.BlockSpec((rb, d), lambda i: (i, 0)), pl.BlockSpec((1, d), lambda i: (0, 0))],
            out_specs=pl.BlockSpec((rb, d), lambda i: (i, 0)), out_shape=xn_shape,
            compiler_params=_params(), cost_estimate=_cost(2e9, 8e6), name="norm",
        )(xa, g2)
        xn_pa = partner(xn_a)
        q_same, q_cross, a_same, a_cross = pl.pallas_call(
            _qkv_next,
            grid_spec=pltpu.PrefetchScalarGridSpec(
                num_scalar_prefetch=1, grid=(3, 2),
                in_specs=[whole, pl.BlockSpec((1, d, 2 * dh), lambda c, i, s: (c, 0, (i + s[ME]) % 2)),
                          tab_spec(0, 1), tab_spec(1, 1)],
                out_specs=[pl.BlockSpec((1, 2, t, dh), lambda *_: (0, 0, 0, 0))] * 2
                + [pl.BlockSpec((1, 2, t, dh), lambda c, *_: (jnp.maximum(c - 1, 0), 0, 0, 0))] * 2,
                scratch_shapes=[pltpu.VMEM((t, 2 * dh), F32)]),
            out_shape=[jax.ShapeDtypeStruct((n, 2, t, dh), BF) for n in (1, 1, 2, 2)],
            compiler_params=_params(), cost_estimate=_cost(flops * 1.4, 35e6), name="qkv_next",
        )(ids, xn_a, w_b, tab, tab)
        rs_a, rc_a = send(a_same, to_same), send(a_cross, to_cross)
        rs_q, rc_q = send(q_same, to_same), send(q_cross, to_cross)
        loc_r = own((xn_po, xn_a, xn_pa), ((1, 0), (0, 1), (1, 1)), ptab)

        def attend(ms):
            nq = len(ms)
            return pl.pallas_call(
                functools.partial(_attend, ms),
                grid_spec=pltpu.PrefetchScalarGridSpec(
                    num_scalar_prefetch=1, grid=(1,),
                    in_specs=[anyspec] * 8,
                    out_specs=[pl.BlockSpec((t, 2 * dh), lambda i, s: (0, 0))] * (2 * nq),
                    scratch_shapes=[pltpu.VMEM((3, 2, 8 * t, dh), BF),
                                    pltpu.VMEM((2, 2 * t, 128), F32), pltpu.VMEM((2, 2 * t, 128), F32),
                                    pltpu.VMEM((2, 2 * t, dh), F32), pltpu.SemaphoreType.DMA((2, 8))]),
                out_shape=[jax.ShapeDtypeStruct((t, 2 * dh), BF)] * (2 * nq),
                compiler_params=_params(), cost_estimate=_cost(nq * 10e9, 13e6), name="attend",
            )(ids, loc_o, loc_r, rs_own, rs_a, rc_own, rc_a, *((rs_q, rc_q) if 6 in ms else (rs_a, rc_a)))

        got = {}
        for ms in GROUPS:
            o = attend(ms)
            for i, m in enumerate(ms):
                for e in range(2):
                    v = m ^ e
                    got[v] = send(o[2 * i + e], lambda j, v=v: j ^ v) if v else o[2 * i + e]

        wo2 = wo.reshape(hh * dh, d)
        o_spec = pl.BlockSpec((t, 2 * dh), lambda i, s: (0, 0))

        def project(tn, ms, part=None):
            n = len(ms)

            def w_spec(m):
                return pl.BlockSpec((2 * dh, tn), lambda i, s: (s[DEV + m], i))

            col = pl.BlockSpec((t, tn), lambda i, s: (0, i))
            kept = pl.BlockSpec(memory_space=pltpu.VMEM)
            return pl.pallas_call(
                functools.partial(_project, n),
                grid_spec=pltpu.PrefetchScalarGridSpec(
                    num_scalar_prefetch=1, grid=(d // tn,),
                    in_specs=[o_spec] * n + [w_spec(m) for m in ms] + [col if part is None else kept],
                    out_specs=kept if part is None else col),
                out_shape=pltpu.VMEM((t, d), F32) if part is None else jax.ShapeDtypeStruct((t, d), BF),
                compiler_params=_params(PROJ_VMEM), cost_estimate=_cost(n * 2 * t * 2 * dh * d * 1.3, n * 4.2e6 + 8e6),
                name="project",
            )(ids, *[got[m] for m in ms], *[wo2] * n, x if part is None else part)

        part = project(TN0, (0, 1, 2, 3, 4, 5))
        return project(TN1, (6, 7), part)

    return jax.shard_map(local, mesh=mesh,
                         in_specs=(rows, P(None), P(None, None, None, None), P(None, None, None)),
                         out_specs=rows, check_vma=False)
```

```python
import functools

import jax
import jax.numpy as jnp
from jax import lax
from jax.experimental import pallas as pl
from jax.experimental.pallas import tpu as pltpu
from jax.sharding import PartitionSpec as P


BF = jnp.bfloat16
F32 = jnp.float32
VMEM_LIMIT = 62 << 20
PROJ_VMEM = KEEP_VMEM = 40 << 20
ATT_VMEM = 50 << 20
OWN_VMEM = 48 << 20
COST = 0.05
TN0, TN1 = 1024, 1024
GROUPS = ((2, 4), (6, 0))
ME, B_HEAD, OWN_HEAD, SRC, DEV = 0, 1, 2, 3, 11


def _norm(x_ref, g_ref, xn):
    rb, d = 16, x_ref.shape[1]
    cols = [slice(j * 128, (j + 1) * 128) for j in range(d // 128)]

    def body(i, carry):
        r = pl.ds(pl.multiple_of(i * rb, rb), rb)
        parts = [jnp.zeros((rb, 128), F32)] * 4
        for j, c in enumerate(cols):
            v = x_ref[r, c].astype(F32)
            parts[j % 4] = parts[j % 4] + v * v
        ss = jnp.sum((parts[0] + parts[1]) + (parts[2] + parts[3]), axis=-1, keepdims=True)
        inv = jnp.broadcast_to(lax.rsqrt(ss * (1.0 / d) + 1e-5), (rb, 128))
        for c in cols:
            xn[r, c] = (x_ref[r, c].astype(F32) * inv * g_ref[:, c]).astype(BF)
        return carry

    lax.fori_loop(0, x_ref.shape[0] // rb, body, 0, unroll=8)


def _norm_rows(x_ref, g_ref, o_ref, keep):
    rb = x_ref.shape[0]
    _norm(x_ref, g_ref, o_ref)
    keep[pl.ds(pl.multiple_of(pl.program_id(0) * rb, rb), rb), :] = o_ref[...]


def _emit_heads(acc, cos, sin, is_v, outs):
    @pl.when(is_v)
    def _():
        for j, o in enumerate(outs):
            o[...] = acc[:, j * 256:(j + 1) * 256].astype(BF)

    @pl.when(jnp.logical_not(is_v))
    def _():
        cs, sn = cos[...], sin[...]
        for j, o in enumerate(outs):
            x1, x2 = acc[:, j * 256:j * 256 + 128], acc[:, j * 256 + 128:(j + 1) * 256]
            o[:, :128] = (x1 * cs - x2 * sn).astype(BF)
            o[:, 128:] = (x2 * cs + x1 * sn).astype(BF)


def _stream(w_ref, buf, sem, head):
    c, d = pl.program_id(0), pl.program_id(1)
    nc, nd = pl.num_programs(0), pl.num_programs(1)
    _, bd, n, dh = buf.shape
    i = c * nd + d

    def copy(j):
        rows = pl.ds(pl.multiple_of(lax.rem(j, nd) * bd, bd), bd)
        heads = pl.ds(pl.multiple_of(head, n), n)
        return pltpu.make_async_copy(w_ref.at[rows, j // nd, heads, :], buf.at[j % 2], sem.at[j % 2])

    @pl.when(i == 0)
    def _():
        copy(0).start()

    @pl.when(i + 1 < nc * nd)
    def _():
        copy(i + 1).start()

    def take():
        copy(i).wait()
        return buf[i % 2].reshape(bd, n * dh)

    return take


def _qkv_first(ids, x_ref, g_ref, w_ref, cos_ref, sin_ref, s_ref, c_ref, o_ref, wr_ref, xn, acc, acc2, wt,
               buf, wsem, buf2, wsem2):
    c, d = pl.program_id(0), pl.program_id(1)
    bd = buf.shape[1]
    take = _stream(w_ref, buf, wsem, ids[B_HEAD])
    take2 = _stream(w_ref, buf2, wsem2, ids[OWN_HEAD])

    @pl.when((c == 0) & (d == 0))
    def _():
        _norm(x_ref, g_ref, xn)

    @pl.when(d == 0)
    def _():
        acc[...] = jnp.zeros_like(acc)
        acc2[...] = jnp.zeros_like(acc2)

    wr_ref[0] = take()
    xb = xn[:, pl.ds(pl.multiple_of(d * bd, bd), bd)]
    acc[...] += jnp.dot(xb, wr_ref[0], preferred_element_type=F32)
    wt[...] = take2()
    acc2[...] += jnp.dot(xb, wt[...], preferred_element_type=F32)

    @pl.when(d == pl.num_programs(1) - 1)
    def _():
        k = ids[ME] % 2
        for o, kk in ((s_ref, k), (c_ref, 1 - k)):
            pair = acc.at[:, pl.ds(pl.multiple_of(kk * 512, 512), 512)]
            _emit_heads(pair, cos_ref, sin_ref, c == 2, [o.at[0, h] for h in range(2)])
        _emit_heads(acc2, cos_ref, sin_ref, c == 2, [o_ref.at[0, h] for h in range(2)])


def _qkv_own(halves, ids, *refs):
    nb = len(halves)
    xr = refs[:nb]
    w_ref, tab_ref, ptab_ref, o_ref, xs, acc, wt, sem, buf, wsem = refs[nb:]
    c, d = pl.program_id(0), pl.program_id(1)
    nd = pl.num_programs(1)
    bd, t = buf.shape[1], xr[0].shape[0]
    take = _stream(w_ref, buf, wsem, ids[OWN_HEAD])

    def copy(b, k):
        cols = pl.ds(pl.multiple_of(k * bd, bd), bd)
        return pltpu.make_async_copy(xr[b].at[:, cols], xs.at[pl.ds(b * t, t), cols], sem.at[k, b])

    @pl.when((c == 0) & (d == 0))
    def _():
        for k in range(xr[0].shape[1] // bd):
            for b in range(nb):
                copy(b, k).start()

    @pl.when(d == 0)
    def _():
        acc[...] = jnp.zeros_like(acc)

    @pl.when(c == 0)
    def _():
        for b in range(nb):
            copy(b, d).wait()

    wt[...] = take()
    cols = pl.ds(pl.multiple_of(d * bd, bd), bd)
    acc[...] += jnp.dot(xs[:, cols], wt[...], preferred_element_type=F32)

    @pl.when(d == nd - 1)
    def _():
        for b, (n, half) in enumerate(halves):
            tb = (tab_ref, ptab_ref)[n]
            r, tr = pl.ds(b * t, t), pl.ds(half * t, t)
            _emit_heads(acc.at[r], tb.at[0, tr], tb.at[1, tr], c == 2, [o_ref.at[b, 0, h] for h in range(2)])


def _qkv_next(ids, xn, w_ref, cos_ref, sin_ref, qs_ref, qc_ref, s_ref, c_ref, acc):
    c, j = pl.program_id(0), pl.program_id(1)
    acc[...] = jnp.dot(xn[...], w_ref[0], preferred_element_type=F32)
    for n, (q_ref, o_ref) in enumerate(((qs_ref, s_ref), (qc_ref, c_ref))):
        @pl.when((j == n) & (c == 0))
        def _():
            _emit_heads(acc, cos_ref, sin_ref, c == 2, [q_ref.at[0, h] for h in range(2)])

        @pl.when((j == n) & (c > 0))
        def _():
            _emit_heads(acc, cos_ref, sin_ref, c == 2, [o_ref.at[0, h] for h in range(2)])


def _attend(masks, ids, lo, lr, rs0, rs1, rc0, rc1, qs1, qc1, *refs):
    nq = len(masks)
    outs = refs[:2 * nq]
    qkv, m_s, l_s, acc, sem = refs[2 * nq:]
    kv = pl.ds(1, 2)
    q_src = [lo.at[0]] + [lr.at[b, 0] for b in range(3)] + [rs0.at[0], qs1.at[0], rc0.at[0], qc1.at[0]]
    kv_src = [lo.at[kv]] + [lr.at[b, kv] for b in range(3)] + [rs0.at[kv], rs1, rc0.at[kv], rc1]
    t, dh = rs0.shape[2:]
    me = ids[ME]
    chips = [(me ^ m) // 2 for m in masks]
    last = functools.reduce(jnp.maximum, chips)

    def kv_copy(n, b):
        rows = pl.ds(pl.multiple_of(b * t, t), t)
        return pltpu.make_async_copy(kv_src[n], qkv.at[kv, :, rows, :], sem.at[0, b])

    def q_copy(n, b):
        rows = pl.ds(pl.multiple_of(b * t, t), t)
        return pltpu.make_async_copy(q_src[n], qkv.at[0, :, rows, :], sem.at[1, b])

    def issue(want_chip, queries):
        for n in range(8):
            b = ids[SRC + n]

            @pl.when(b // 2 == want_chip)
            def _():
                if queries:
                    q_copy(n, b).start()
                else:
                    kv_copy(n, b).start()

    issue(chips[0], True)
    for j in range(4):
        @pl.when(j <= last)
        def _():
            issue(j, False)

        if j == 0:
            for cc in chips[1:]:
                issue(cc, True)

    k2 = (dh ** -0.5) * 1.4426950408889634

    k = me % 2

    def chip_rows(i, carry):
        cc = jnp.where(i == 0, chips[0], chips[1])
        q0 = pl.multiple_of(cc * 2 * t, 2 * t)
        for b in range(2):
            q_copy(0, 2 * cc + b).wait()
        m_s[...] = jnp.full_like(m_s, -jnp.inf)
        l_s[...] = jnp.zeros_like(l_s)
        acc[...] = jnp.zeros_like(acc)

        def kv_wait(j):
            @pl.when(i == 0)
            def _():
                for b in range(2):
                    kv_copy(0, 2 * j + b).wait()

        def tile(base, r0, nr, w, masked):
            rs = slice(r0, r0 + nr)
            ss = []
            for h in range(2):
                s = lax.dot_general(qkv[0, h, pl.ds(q0 + r0, nr), :], qkv[1, h, pl.ds(base, w), :],
                                    (((1,), (1,)), ((), ())), preferred_element_type=F32)
                if masked:
                    row = lax.broadcasted_iota(jnp.int32, (nr, w), 0)
                    col = lax.broadcasted_iota(jnp.int32, (nr, w), 1)
                    s = jnp.where(row >= col, s, -jnp.inf)
                ss.append(s)
            for h in range(2):
                ch = [ss[h][:, q * 128:(q + 1) * 128] for q in range(w // 128)]
                m_old = m_s[h, rs]
                m_new = jnp.maximum(m_old, jnp.max(functools.reduce(jnp.maximum, ch), axis=-1, keepdims=True))
                alpha = jnp.exp2((m_old - m_new) * k2)
                m_s[h, rs] = m_new
                mk = m_new * k2
                ps = [jnp.exp2(v * k2 - mk) for v in ch]
                l_s[h, rs] = l_s[h, rs] * alpha + functools.reduce(jnp.add, ps)
                p = jnp.concatenate([v.astype(BF) for v in ps], axis=1)
                pv = jnp.dot(p, qkv[2, h, pl.ds(base, w), :], preferred_element_type=F32)
                for q in range(dh // 128):
                    sl = slice(q * 128, (q + 1) * 128)
                    acc[h, rs, sl] = acc[h, rs, sl] * alpha + pv[:, sl]

        def body(j, carry):
            kv_wait(j)
            tile(pl.multiple_of(j * 2 * t, 2 * t), 0, 2 * t, 2 * t, False)
            return carry

        lax.fori_loop(0, cc, body, 0)
        kv_wait(cc)
        tile(q0, 0, t, t, True)
        tile(q0, t, t, t, False)
        tile(pl.multiple_of(q0 + t, t), t, t, t, True)

        @pl.when(i == 0)
        def _():
            def drain(j, carry):
                kv_wait(j)
                return carry

            lax.fori_loop(cc + 1, last + 1, drain, 0)

        for o in range(2):
            rs = pl.ds(pl.multiple_of((k if o == 0 else 1 - k) * t, t), t)
            for h in range(2):
                l = jnp.sum(l_s[h, rs, :], axis=-1, keepdims=True)
                v = (acc[h, rs, :] / l).astype(BF)
                for n in range(nq):
                    @pl.when(i == n)
                    def _(n=n):
                        outs[2 * n + o][:, h * dh:(h + 1) * dh] = v
        return carry

    lax.fori_loop(0, nq, chip_rows, 0)


def _project(n, ids, *refs):
    o = jnp.concatenate([r[...] for r in refs[:n]], axis=1)
    w = jnp.concatenate([r[...] for r in refs[n:2 * n]], axis=0)
    base, out = refs[2 * n], refs[2 * n + 1]
    tn = w.shape[1]
    cols = pl.ds(pl.multiple_of(pl.program_id(0) * tn, tn), tn)
    a = jnp.dot(o, w, preferred_element_type=F32)
    if out.shape[1] == tn:
        out[...] = (base[:, cols] + a).astype(BF)
    else:
        out[:, cols] = base[...].astype(F32) + a


def _params(limit=VMEM_LIMIT):
    return pltpu.CompilerParams(vmem_limit_bytes=limit)


def _cost(flops, nbytes):
    return pl.CostEstimate(flops=int(flops * COST), bytes_accessed=int(nbytes * COST), transcendentals=0)


def solution(mesh):
    rows = P(("data", "seq"), None)

    def local(x, g, wqkv, wo):
        t, d = x.shape
        _, _, hh, dh = wqkv.shape
        me = lax.axis_index("seq").astype(jnp.int32)
        k = me % 2
        kf, yf = 2 << k, 4 >> k

        def send(a, f):
            return lax.ppermute(a, "seq", [(i, f(i)) for i in range(8)])

        def to_a(i):
            return i ^ (2 << (i & 1))

        def to_same(i):
            return i ^ (4 >> (i & 1))

        def to_cross(i):
            return to_same(i) ^ 1

        inv = 10000.0 ** (-jnp.arange(dh // 2, dtype=F32) * 2.0 / dh)

        def tables(b):
            pos = (b[:, None] * t + jnp.arange(t)[None, :]).reshape(-1).astype(F32)
            ang = pos[:, None] * inv[None, :]
            return jnp.stack([jnp.cos(ang), jnp.sin(ang)])

        a_id, so, po = me ^ kf, me ^ yf, me ^ 1
        xo = po ^ kf

        ids = jnp.stack([me, so // 2 * 4, me * 2]
                        + [me, po, a_id, po ^ yf, so, me ^ 6, xo, me ^ 7]
                        + [me ^ m for m in range(8)]).astype(jnp.int32)
        tab = tables(jnp.stack([me, a_id]))
        g2 = g[None, :]

        xa = send(x, to_a)

        half = jax.ShapeDtypeStruct((3, 2, t, dh), BF)
        xn_shape = jax.ShapeDtypeStruct((t, d), BF)
        bd = 1024
        nd = d // bd
        flops = 2 * t * d * 12 * dh

        def partner(a):
            return send(a, lambda i: i ^ 1)

        def tiles(n):
            return [pltpu.VMEM((2, bd, n, dh), BF), pltpu.SemaphoreType.DMA((2,))]

        def tab_spec(n, b):
            return pl.BlockSpec((pl.Squeezed(), t, dh // 2), lambda *_: (n, b, 0))

        whole = pl.BlockSpec((t, d), lambda *_: (0, 0), pipeline_mode=pl.Buffered(1))
        anyspec = pl.BlockSpec(memory_space=pl.ANY)
        half2 = pl.BlockSpec((1, 2, t, dh), lambda c, *_: (c, 0, 0, 0))

        b_same, b_cross, loc_o, w_b, xn_o = pl.pallas_call(
            _qkv_first,
            grid_spec=pltpu.PrefetchScalarGridSpec(
                num_scalar_prefetch=1, grid=(3, nd),
                in_specs=[whole, pl.BlockSpec((1, d), lambda *_: (0, 0)), anyspec,
                          tab_spec(0, 0), tab_spec(1, 0)],
                out_specs=[half2, half2, half2, pl.BlockSpec((1, bd, 4 * dh), lambda c, i, s: (c, i, 0)), whole],
                scratch_shapes=[pltpu.VMEM((t, 4 * dh), F32), pltpu.VMEM((t, 2 * dh), F32),
                                pltpu.VMEM((bd, 2 * dh), BF)] + tiles(4) + tiles(2)),
            out_shape=[half, half, half, jax.ShapeDtypeStruct((3, d, 4 * dh), BF), xn_shape],
            compiler_params=_params(), cost_estimate=_cost(flops * 2.5, 80e6), name="qkv_first",
        )(ids, x, g2, wqkv, tab, tab)
        both_tab = pl.BlockSpec((2, 2 * t, dh // 2), lambda *_: (0, 0, 0), pipeline_mode=pl.Buffered(1))

        def own(xs, halves, ptab):
            n = len(xs)
            return pl.pallas_call(
                functools.partial(_qkv_own, halves),
                grid_spec=pltpu.PrefetchScalarGridSpec(
                    num_scalar_prefetch=1, grid=(3, 2),
                    in_specs=[anyspec] * (n + 1) + [both_tab, both_tab],
                    out_specs=pl.BlockSpec((n, 1, 2, t, dh), lambda c, i, s: (0, c, 0, 0, 0)),
                    scratch_shapes=[pltpu.VMEM((n * t, d), BF), pltpu.VMEM((n * t, 2 * dh), F32),
                                    pltpu.VMEM((2048, 2 * dh), BF), pltpu.SemaphoreType.DMA((2, n))]
                    + [pltpu.VMEM((2, 2048, 2, dh), BF), pltpu.SemaphoreType.DMA((2,))]),
                out_shape=jax.ShapeDtypeStruct((n, 3, 2, t, dh), BF),
                compiler_params=_params(OWN_VMEM), cost_estimate=_cost(flops * 0.7 * n, 15e6 + n * 6e6), name="qkv_own",
            )(ids, *xs, wqkv, tab, ptab)

        rs_own, rc_own = send(b_same, to_same), send(b_cross, to_cross)
        xn_po, ptab = partner(xn_o), partner(tab)
        rb = 256
        kept = pl.BlockSpec(memory_space=pltpu.VMEM)
        xn_a, xn_k = pl.pallas_call(
            _norm_rows, grid=(t // rb,),
            in_specs=[pl.BlockSpec((rb, d), lambda i: (i, 0)), pl.BlockSpec((1, d), lambda i: (0, 0))],
            out_specs=[pl.BlockSpec((rb, d), lambda i: (i, 0)), kept],
            out_shape=[xn_shape, pltpu.VMEM((t, d), BF)],
            compiler_params=_params(KEEP_VMEM), cost_estimate=_cost(2e9, 8e6), name="norm",
        )(xa, g2)
        xn_pa = partner(xn_a)
        q_same, q_cross, a_same, a_cross = pl.pallas_call(
            _qkv_next,
            grid_spec=pltpu.PrefetchScalarGridSpec(
                num_scalar_prefetch=1, grid=(3, 2),
                in_specs=[kept, pl.BlockSpec((1, d, 2 * dh), lambda c, i, s: (c, 0, (i + s[ME]) % 2)),
                          tab_spec(0, 1), tab_spec(1, 1)],
                out_specs=[pl.BlockSpec((1, 2, t, dh), lambda *_: (0, 0, 0, 0))] * 2
                + [pl.BlockSpec((1, 2, t, dh), lambda c, *_: (jnp.maximum(c - 1, 0), 0, 0, 0))] * 2,
                scratch_shapes=[pltpu.VMEM((t, 2 * dh), F32)]),
            out_shape=[jax.ShapeDtypeStruct((n, 2, t, dh), BF) for n in (1, 1, 2, 2)],
            compiler_params=_params(KEEP_VMEM), cost_estimate=_cost(flops * 1.4, 35e6), name="qkv_next",
        )(ids, xn_k, w_b, tab, tab)
        rs_a, rc_a = send(a_same, to_same), send(a_cross, to_cross)
        rs_q, rc_q = send(q_same, to_same), send(q_cross, to_cross)
        loc_r = own((xn_po, xn_a, xn_pa), ((1, 0), (0, 1), (1, 1)), ptab)

        def attend(ms):
            nq = len(ms)
            return pl.pallas_call(
                functools.partial(_attend, ms),
                grid_spec=pltpu.PrefetchScalarGridSpec(
                    num_scalar_prefetch=1, grid=(1,),
                    in_specs=[anyspec] * 8,
                    out_specs=[kept if m == 0 and e == 0 else pl.BlockSpec((t, 2 * dh), lambda i, s: (0, 0))
                               for m in ms for e in range(2)],
                    scratch_shapes=[pltpu.VMEM((3, 2, 8 * t, dh), BF),
                                    pltpu.VMEM((2, 2 * t, 128), F32), pltpu.VMEM((2, 2 * t, 128), F32),
                                    pltpu.VMEM((2, 2 * t, dh), F32), pltpu.SemaphoreType.DMA((2, 8))]),
                out_shape=[(pltpu.VMEM if m == 0 and e == 0 else jax.ShapeDtypeStruct)((t, 2 * dh), BF)
                           for m in ms for e in range(2)],
                compiler_params=_params(ATT_VMEM), cost_estimate=_cost(nq * 10e9, 13e6), name="attend",
            )(ids, loc_o, loc_r, rs_own, rs_a, rc_own, rc_a, *((rs_q, rc_q) if 6 in ms else (rs_a, rc_a)))

        got = {}
        for ms in GROUPS:
            o = attend(ms)
            for i, m in enumerate(ms):
                for e in range(2):
                    v = m ^ e
                    got[v] = send(o[2 * i + e], lambda j, v=v: j ^ v) if v else o[2 * i + e]

        wo2 = wo.reshape(hh * dh, d)
        o_spec = pl.BlockSpec((t, 2 * dh), lambda i, s: (0, 0))

        def project(tn, ms, part=None):
            n = len(ms)

            def w_spec(m):
                return pl.BlockSpec((2 * dh, tn), lambda i, s: (s[DEV + m], i))

            col = pl.BlockSpec((t, tn), lambda i, s: (0, i))
            return pl.pallas_call(
                functools.partial(_project, n),
                grid_spec=pltpu.PrefetchScalarGridSpec(
                    num_scalar_prefetch=1, grid=(d // tn,),
                    in_specs=[o_spec if m else kept for m in ms] + [w_spec(m) for m in ms] + [col if part is None else kept],
                    out_specs=kept if part is None else col),
                out_shape=pltpu.VMEM((t, d), F32) if part is None else jax.ShapeDtypeStruct((t, d), BF),
                compiler_params=_params(PROJ_VMEM), cost_estimate=_cost(n * 2 * t * 2 * dh * d * 1.3, n * 4.2e6 + 8e6),
                name="project",
            )(ids, *[got[m] for m in ms], *[wo2] * n, x if part is None else part)

        part = project(TN0, (0, 1, 2, 3, 4, 5))
        return project(TN1, (6, 7), part)

    return jax.shard_map(local, mesh=mesh,
                         in_specs=(rows, P(None), P(None, None, None, None), P(None, None, None)),
                         out_specs=rows, check_vma=False)
```
